32 devices in a mesh: psr: 8 (over z, x), toa: 4 (over y, core).
Axes of the slice: x: 2, y: 2, z: 4, core: 2. Of those that a mesh axis runs over, the one named last changes fastest.
Arguments:
- design: bfloat16 [3072, 128, 256], P(('psr', 'toa')), may hold values from -0.035888672 to 0.035888672
- noise_weight: float32 [3072, 128], P(('psr', 'toa')), may hold values from 0.3 to 3
- residuals: bfloat16 [3072, 128], P(('psr', 'toa')), may hold values from -6 to 6
- slot_pulsar: int32 [3072], P(('psr', 'toa')), may hold values from 0 to 7, as said below
- slot_rows: int32 [3072], P(('psr', 'toa')), may hold values from 0 to 128, as said below
- own_prior: float32 [64, 192], P(('psr', 'toa')), may hold values from 0.2 to 5
- spectrum: float32 [32], replicated, may hold values from 0.05 to 2
- directions: float32 [3, 64], replicated, may hold values from -1 to 1, as said below
Outputs:
- coeffs: float32 [64, 64], P(('psr', 'toa'))
- log_dets: float32 [64], P(('psr', 'toa'))
- chi_square: float32 [64], P(('psr', 'toa'))
The draws below stay inside these ranges and needn't reach their ends.
Inputs may be any that keep to these rules, and one draw needn't show every extreme that they name: `slot_pulsar`: pulsar k of group g is pulsar g * 8 + k of the arrays with a pulsar dimension; empty blocks name pulsar 0. `slot_rows`: on each device the blocks holding TOAs come first and the empty ones (0 rows) last; within a psr group a pulsar's blocks are consecutive in device order, cyclically, all full but its last; every pulsar has between 4 * 96 * 4 and 4 * 96 * 16 TOAs. `directions`: unit vectors; any two are at least 0.1 radians apart.
All inputs are finite; a program needn't handle non-finite values.
Results may differ from the reference program's by a relative error of at most 0.003.
Values sent between devices are 32-bit elements; how exact they have to be, the bound alone decides.
A program may use at most 128 MiB of HBM per device.

```python
import math
import jax
import jax.numpy as jnp
from jax import lax

GROUP_PULSARS = 8
PULSARS = 64
COLUMNS = 256
FREQS = 32
OWN = 192
BLOCK_ROWS = 128
SLOTS = 96
BLOCKS = 3072
ITERS = 8
N_PSR = 8
N_TOA = 4


def slot_layout(key):
    capacity = N_TOA * SLOTS
    pulsar_cap = capacity * BLOCK_ROWS // GROUP_PULSARS
    toa_counts = jax.random.randint(jax.random.fold_in(key, 101), (N_PSR, GROUP_PULSARS), pulsar_cap // 4, pulsar_cap + 1)
    blocks = (toa_counts + BLOCK_ROWS - 1) // BLOCK_ROWS
    block_ends = jnp.cumsum(blocks, axis=1)
    begins = block_ends - blocks
    first_device = jax.random.randint(jax.random.fold_in(key, 102), (N_PSR, 1), 0, N_TOA)
    position = jnp.arange(capacity, dtype=jnp.int32)[None, :]
    group_block = (position - first_device * SLOTS) % capacity
    inside = (group_block[:, :, None] >= begins[:, None, :]) & (group_block[:, :, None] < block_ends[:, None, :])
    serial = jnp.arange(GROUP_PULSARS, dtype=jnp.int32)[None, None, :]
    pulsar = jnp.sum(jnp.where(inside, serial, 0), axis=2)
    filled = jnp.any(inside, axis=2)
    last_block = jnp.sum(jnp.where(inside, (block_ends - 1)[:, None, :], 0), axis=2)
    tail_rows = jnp.sum(jnp.where(inside, (toa_counts - BLOCK_ROWS * (blocks - 1))[:, None, :], 0), axis=2)
    row_count = jnp.where(filled, jnp.where(group_block == last_block, tail_rows, BLOCK_ROWS), 0)
    return (pulsar.reshape(-1).astype(jnp.int32), row_count.reshape(-1).astype(jnp.int32))


def draw_slot_pulsar(key, part):
    return slot_layout(key)[0]


def draw_slot_rows(key, part):
    return slot_layout(key)[1]


def draw_directions(key, part):
    clusters = N_PSR
    members = GROUP_PULSARS
    number = clusters * members
    serial = jnp.arange(clusters).astype(jnp.float32)
    offset_angle = jax.random.uniform(jax.random.fold_in(key, 201), (), jnp.float32, 0.0, 6.2831853)
    height = 1.0 - (2.0 * serial + 1.0) / clusters
    azimuth = 2.39996323 * serial + offset_angle
    radius = jnp.sqrt(jnp.maximum(1.0 - height * height, 0.0))
    centre = jnp.stack([radius * jnp.cos(azimuth), radius * jnp.sin(azimuth), height], axis=1)
    east_axis = jnp.stack([-jnp.sin(azimuth), jnp.cos(azimuth), jnp.zeros_like(azimuth)], axis=1)
    north_axis = jnp.cross(centre, east_axis)
    cycle_size = jax.random.uniform(jax.random.fold_in(key, 202), (clusters, 1), jnp.float32, 0.135, 0.16)
    cycle_turn = jax.random.uniform(jax.random.fold_in(key, 203), (clusters, 1), jnp.float32, 0.0, 6.2831853)
    spoke_shake = jax.random.uniform(jax.random.fold_in(key, 204), (clusters, members), jnp.float32, -0.03, 0.03)
    radial_shake = jax.random.uniform(jax.random.fold_in(key, 205), (clusters, members), jnp.float32, 0.97, 1.03)
    member_index = jnp.arange(members).astype(jnp.float32)[None, :]
    spoke_angle = 6.2831853 * (member_index - 1.0) / (members - 1) + cycle_turn + spoke_shake
    distance = jnp.where(member_index > 0.5, cycle_size * radial_shake, 0.0)
    across = jnp.cos(spoke_angle)[:, :, None] * east_axis[:, None, :] + jnp.sin(spoke_angle)[:, :, None] * north_axis[:, None, :]
    points = jnp.cos(distance)[:, :, None] * centre[:, None, :] + jnp.sin(distance)[:, :, None] * across
    points = points.reshape((number, 3)).T
    shuffle = jax.random.permutation(jax.random.fold_in(key, 206), number)
    return points[:, shuffle].astype(jnp.float32)


def levels(rng, extent, split, smallest, largest):
    factor_of, own = 1.0, jax.random.fold_in(rng, 6)
    for axis_at, parts in split:
        draws = jnp.exp(jax.random.uniform(jax.random.fold_in(own, axis_at), (parts,), jnp.float32, smallest / len(split), largest / len(split)))
        factor_of = factor_of * jnp.repeat(draws, extent[axis_at] // parts).reshape([-1 if axis == axis_at else 1 for axis in range(len(extent))])
    return factor_of


def bell_draw(stream_key, dims, deviation, bound, cuts=(), held_as=jnp.bfloat16):
    level = levels(stream_key, dims, cuts, -0.22, 0.18) if cuts else 1.0
    array = jax.random.normal(stream_key, dims, jnp.float32) * deviation * level
    return jnp.minimum(jnp.maximum(array, -bound), bound).astype(held_as)


def setup_inputs(seed: int = 0) -> dict:
    keys = jax.random.split(jax.random.key(seed), 9)
    return {
        "design": bell_draw(keys[0], (BLOCKS, BLOCK_ROWS, COLUMNS), 0.006, 0.035888672, ((0, 32),)),
        "noise_weight": jnp.clip(jnp.exp(math.log(3.0) - 2.3025851 * jax.random.uniform(keys[1], (BLOCKS, BLOCK_ROWS), jnp.float32) ** levels(keys[1], (BLOCKS, BLOCK_ROWS), ((0, 32),), -0.2, 0.2)), 0.3, 3.0),
        "residuals": bell_draw(keys[2], (BLOCKS, BLOCK_ROWS), 1.0, 6.0, ((0, 32),)),
        "slot_pulsar": draw_slot_pulsar(jax.random.fold_in(keys[8], 71), 0),
        "slot_rows": draw_slot_rows(jax.random.fold_in(keys[8], 71), 0),
        "own_prior": jnp.clip(jnp.exp(math.log(5.0) - 3.218876 * jax.random.uniform(keys[5], (PULSARS, OWN), jnp.float32) ** levels(keys[5], (PULSARS, OWN), ((0, 32),), -0.2, 0.2)), 0.2, 5.0),
        "spectrum": jnp.clip(jnp.exp(jax.random.uniform(keys[6], (FREQS,), jnp.float32, math.log(0.05), math.log(2.0))), 0.05, 2.0),
        "directions": draw_directions(jax.random.fold_in(keys[8], 71), 0),
    }


highest = lax.Precision.HIGHEST

def cholesky_solve(factor, right_side):
    halfway = lax.linalg.triangular_solve(factor, right_side, left_side=True, lower=True)
    return lax.linalg.triangular_solve(factor, halfway, left_side=True, lower=True, transpose_a=True)

def slot_term_values(design, weight, residuals, pulsar, slot_rows):
    positions = lax.broadcasted_iota(jnp.int32, weight.shape, 1)
    weight = jnp.where(positions < slot_rows[:, None], weight, 0.0)
    weighted = (weight[:, :, None] * design.astype(jnp.float32)).astype(jnp.bfloat16)
    weighted = lax.optimization_barrier(weighted)
    wide_weighted = weighted.astype(jnp.float32)
    wide_design = design.astype(jnp.float32)
    wide_residual = residuals.astype(jnp.float32)
    products = jnp.einsum('srk,srl->skl', wide_weighted, wide_design, precision=highest)
    fitted = jnp.einsum('srk,sr->sk', wide_weighted, wide_residual, precision=highest)
    energy = jnp.sum(weight * wide_residual * wide_residual, axis=1)
    owners = (pulsar[:, None] == lax.broadcasted_iota(jnp.int32, (pulsar.shape[0], GROUP_PULSARS), 1)).astype(jnp.float32)
    return (jnp.einsum('sp,skl->pkl', owners, products, precision=highest), jnp.einsum('sp,sk->pk', owners, fitted, precision=highest), jnp.dot(energy, owners, precision=highest), jnp.dot(slot_rows.astype(jnp.float32), owners, precision=highest))

def group_grams(design, weight, residuals, pulsar, slot_rows):
    count_blocks = design.shape[0] // 16
    column_count = design.shape[2]

    def regroup(member):
        return member.reshape((count_blocks, 16) + member.shape[1:])

    def one_block(running_total, group_members):
        summand_terms = slot_term_values(*group_members)
        return (tuple((earlier_term + later_term for earlier_term, later_term in zip(running_total, summand_terms))), 0)
    initial = (jnp.zeros((GROUP_PULSARS, column_count, column_count), jnp.float32), jnp.zeros((GROUP_PULSARS, column_count), jnp.float32), jnp.zeros((GROUP_PULSARS,), jnp.float32), jnp.zeros((GROUP_PULSARS,), jnp.float32))
    group_members = tuple((regroup(member) for member in (design, weight, residuals, pulsar, slot_rows)))
    totals, unused = lax.scan(one_block, initial, group_members)
    return totals

def eliminate(gram_sums, projections, own_prior):
    column_count = gram_sums.shape[1]
    common = column_count - own_prior.shape[1]
    identity = jnp.eye(own_prior.shape[1], dtype=jnp.float32)
    own_block = gram_sums[:, common:, common:] + (1.0 / own_prior)[:, :, None] * identity[None, :, :]
    factor = jnp.linalg.cholesky(own_block)
    right_side = jnp.concatenate([gram_sums[:, common:, :common], projections[:, common:, None]], axis=2)
    solved = cholesky_solve(factor, right_side)
    cross_block = gram_sums[:, :common, common:]
    reduced = jnp.einsum('pck,pkd->pcd', cross_block, solved, precision=highest)
    schur_part = gram_sums[:, :common, :common] - reduced[:, :, :common]
    target = projections[:, :common] - reduced[:, :, common]
    quadratic = jnp.sum(projections[:, common:] * solved[:, :, common], axis=1)
    own_logdet = 2.0 * jnp.sum(jnp.log(jnp.diagonal(factor, axis1=1, axis2=2)), axis=1)
    return (schur_part, target, quadratic, own_logdet)

def coupling_inverse(directions):
    cosines = jnp.clip(jnp.dot(directions.T, directions, precision=highest), -1.0, 1.0)
    number = cosines.shape[0]
    diagonal = jnp.eye(number, dtype=jnp.float32) > 0.5
    spread = jnp.where(diagonal, 1.0, 0.5 * (1.0 - cosines))
    intersect_curve = 1.5 * spread * jnp.log(spread) - 0.25 * spread + 0.5
    correlation = jnp.where(diagonal, 1.0, intersect_curve)
    factor = jnp.linalg.cholesky(correlation)
    return cholesky_solve(factor, jnp.eye(number, dtype=jnp.float32))

def coupled_apply(schur_part, coupling, inverse_power, vector):
    within = jnp.einsum('pcd,pd->pc', schur_part, vector, precision=highest)
    mixing = jnp.dot(coupling, vector, precision=highest)
    return within + mixing * inverse_power[None, :]

def precondition(block_factor, residual):
    return cholesky_solve(block_factor, residual[:, :, None])[:, :, 0]

def reference(design, noise_weight, residuals, slot_pulsar, slot_rows, own_prior, spectrum, directions):
    groups = N_PSR
    group_slots = design.shape[0] // groups
    shaped = tuple((member.reshape((groups, group_slots) + member.shape[1:]) for member in (design, noise_weight, residuals, slot_pulsar, slot_rows)))

    def per_group(group_members):
        return group_grams(*group_members)
    gram_sums, projections, energy, counts = lax.map(per_group, shaped)
    gram_sums = gram_sums.reshape((PULSARS, COLUMNS, COLUMNS))
    projections = projections.reshape((PULSARS, COLUMNS))
    energy = energy.reshape((PULSARS,))
    counts = counts.reshape((PULSARS,))
    schur_part, target, quadratic, own_logdet = eliminate(gram_sums, projections, own_prior)
    coupling = coupling_inverse(directions)
    inverse_power = 1.0 / jnp.repeat(spectrum, 2)
    block_matrix = schur_part + jnp.diagonal(coupling)[:, None, None] * jnp.diag(inverse_power)[None, :, :]
    block_factor = jnp.linalg.cholesky(block_matrix)
    block_logdet = 2.0 * jnp.sum(jnp.log(jnp.diagonal(block_factor, axis1=1, axis2=2)), axis=1)
    solution = jnp.zeros_like(target)
    residual = target
    scaled = precondition(block_factor, residual)
    direction = scaled
    inner_now = jnp.sum(residual * scaled)
    for iteration in range(ITERS):
        mapped = coupled_apply(schur_part, coupling, inverse_power, direction)
        step_size = inner_now / jnp.sum(direction * mapped)
        solution = solution + step_size * direction
        residual = residual - step_size * mapped
        if iteration + 1 < ITERS:
            scaled = precondition(block_factor, residual)
            inner_next = jnp.sum(residual * scaled)
            direction = scaled + inner_next / inner_now * direction
            inner_now = inner_next
    log_dets = (own_logdet + block_logdet) / COLUMNS
    chi_square = (energy - quadratic - jnp.sum(target * solution, axis=1)) / counts
    return (solution, log_dets, chi_square)
```

```python
import functools

import jax
import jax.numpy as jnp
from jax import lax
from jax.experimental import pallas as pl
from jax.experimental.pallas import tpu as pltpu
from jax.sharding import PartitionSpec as P

GROUP_PULSARS = 8
ITERS = 8
SIDE = 64
STEP_SLOTS = 8
PANEL = 16
highest = lax.Precision.HIGHEST


def dot(a, b, precision=highest):
    return jnp.dot(a, b, precision=precision, preferred_element_type=jnp.float32)


def gram_kernel(pulsar_ref, rows_ref, design_ref, weight_ref, residual_ref, out_ref):
    step = pl.program_id(0)
    toas, columns = design_ref.shape[1], design_ref.shape[2]

    @pl.when(step == 0)
    def _():
        out_ref[...] = jnp.zeros_like(out_ref)

    lanes = lax.broadcasted_iota(jnp.int32, (1, toas), 1)
    for j in range(STEP_SLOTS):
        slot = step * STEP_SLOTS + j
        p = pulsar_ref[slot]
        valid = lanes < rows_ref[slot]
        weight = jnp.where(valid, weight_ref[j : j + 1, :], 0.0)
        residual = residual_ref[j : j + 1, :].astype(jnp.float32)
        block = design_ref[j]
        across = jnp.transpose(block).astype(jnp.float32)
        weighted = (across * weight).astype(jnp.bfloat16)
        gram = jnp.dot(weighted, block, preferred_element_type=jnp.float32)
        spread = jnp.broadcast_to(residual, (8, toas)).astype(jnp.bfloat16)
        fitted = lax.dot_general(
            spread, weighted, (((1,), (1,)), ((), ())), preferred_element_type=jnp.float32
        )
        energy = weight * residual * residual
        count = jnp.where(valid, 1.0, 0.0)
        tail = jnp.concatenate([energy, count], axis=1)
        at_row = lax.broadcasted_iota(jnp.int32, (8, columns), 0)
        extra = jnp.where(at_row == 0, fitted, jnp.where(at_row == 1, tail, 0.0))
        out_ref[p, 0:columns, :] += gram
        out_ref[p, columns : columns + 8, :] += extra


def local_grams(design, noise_weight, residuals, slot_pulsar, slot_rows):
    slots, toas, columns = design.shape
    return pl.pallas_call(
        gram_kernel,
        grid_spec=pltpu.PrefetchScalarGridSpec(
            num_scalar_prefetch=2,
            grid=(slots // STEP_SLOTS,),
            in_specs=[
                pl.BlockSpec((STEP_SLOTS, toas, columns), lambda i, *_: (i, 0, 0)),
                pl.BlockSpec((STEP_SLOTS, toas), lambda i, *_: (i, 0)),
                pl.BlockSpec((STEP_SLOTS, toas), lambda i, *_: (i, 0)),
            ],
            out_specs=pl.BlockSpec((GROUP_PULSARS, columns + 8, columns), lambda i, *_: (0, 0, 0)),
        ),
        out_shape=jax.ShapeDtypeStruct((GROUP_PULSARS, columns + 8, columns), jnp.float32),
        name="gram",
    )(slot_pulsar, slot_rows, design, noise_weight, residuals)


def invert(mats):
    side = mats[0].shape[0]
    lane = lax.broadcasted_iota(jnp.int32, (1, side), 1)
    sub = lax.broadcasted_iota(jnp.int32, (side, side), 0)
    lane_full = lax.broadcasted_iota(jnp.int32, (side, side), 1)
    pivots = [jnp.ones((1, side), jnp.float32) for _ in mats]
    mats = list(mats)
    for k in range(side):
        for m, a in enumerate(mats):
            row = a[k : k + 1, :]
            col = a[:, k : k + 1]
            pivot = a[k : k + 1, k : k + 1]
            inverse = 1.0 / pivot
            pivots[m] = jnp.where(lane == k, pivot, pivots[m])
            row = jnp.where(lane == k, 1.0, row) * inverse
            kept = jnp.where(lane_full == k, 0.0, a)
            mats[m] = jnp.where(sub == k, row, kept - col * row)
    return mats, [jnp.sum(jnp.log(v), axis=1, keepdims=True) for v in pivots]


def coupling_kernel(directions_ref, out_ref):
    d = directions_ref[...]
    cosines = jnp.clip(
        lax.dot_general(d, d, (((0,), (0,)), ((), ())), precision=highest, preferred_element_type=jnp.float32),
        -1.0,
        1.0,
    )
    number = cosines.shape[0]
    row = lax.broadcasted_iota(jnp.int32, (number, number), 0)
    col = lax.broadcasted_iota(jnp.int32, (number, number), 1)
    spread = jnp.where(row == col, 1.0, 0.5 * (1.0 - cosines))
    curve = 1.5 * spread * jnp.log(spread) - 0.25 * spread + 0.5
    x = jnp.where(row == col, 1.0, curve)
    side = min(SIDE, number)
    for b in range(number // side):
        lo, hi = b * side, (b + 1) * side
        (inverse,), _ = invert([x[lo:hi, lo:hi]])
        if number == side:
            x = inverse
            continue
        across = dot(inverse, x[lo:hi, :])
        down = x[:, lo:hi]
        inside_row = (row >= lo) & (row < hi)
        inside_col = (col >= lo) & (col < hi)
        updated = x - dot(down, across)
        placed = -dot(down, inverse)
        tiles = number // side
        updated = jnp.where(inside_col, jnp.concatenate([placed] * tiles, axis=1), updated)
        fixed = jnp.where(inside_col, jnp.concatenate([jnp.concatenate([inverse] * tiles, axis=1)] * tiles, axis=0),
                          jnp.concatenate([across] * tiles, axis=0))
        x = jnp.where(inside_row, fixed, updated)
    out_ref[...] = x


def coupling_inverse(directions):
    number = directions.shape[1]
    padded = jnp.pad(directions, ((0, 8 - directions.shape[0]), (0, 0)))
    return pl.pallas_call(
        coupling_kernel,
        out_shape=jax.ShapeDtypeStruct((number, number), jnp.float32),
        cost_estimate=pl.CostEstimate(flops=number**3 * 60, bytes_accessed=4 * number * number, transcendentals=0),
        name="coupling",
    )(padded)


def invert_pair(x, width):
    side, lanes = x.shape
    lane = lax.broadcasted_iota(jnp.int32, (1, lanes), 1)
    within = lax.rem(lane, side)
    half = lax.broadcasted_iota(jnp.int32, (side, lanes), 1)
    half = half - lax.rem(half, side)
    pivots = jnp.ones((1, lanes), jnp.float32)
    for lo in range(0, side, width):
        hi = lo + width
        columns = [jnp.take_along_axis(x, half + (lo + k), axis=1) for k in range(width)]
        rows = x[lo:hi]
        inner = [c[lo:hi] for c in columns]
        sub = lax.broadcasted_iota(jnp.int32, (width, lanes), 0)
        for k in range(width):
            here = within == lo + k
            pivot = inner[k][k : k + 1]
            inverse = 1.0 / pivot
            pivots = jnp.where(here, pivot, pivots)
            row = jnp.where(here, 1.0, rows[k : k + 1]) * inverse
            at = sub == k
            rows = jnp.where(at, row, jnp.where(here, 0.0, rows) - inner[k] * row)
            for j in range(k + 1, width):
                scaled = inner[j][k : k + 1] * inverse
                inner[j] = jnp.where(at, scaled, inner[j] - inner[k] * scaled)
        inside = (within >= lo) & (within < hi)
        parts = []
        for begin in range(0, side, width):
            if begin == lo:
                parts.append(rows)
                continue
            acc = jnp.where(inside, 0.0, x[begin : begin + width])
            for k in range(width):
                acc = acc - columns[k][begin : begin + width] * rows[k : k + 1]
            parts.append(acc)
        x = jnp.concatenate(parts, axis=0)
    return x, jnp.log(pivots)


def paired(block):
    side, lanes = block.shape
    lane = lax.broadcasted_iota(jnp.int32, (side, lanes), 1)
    return jnp.concatenate([jnp.where(lane < side, block, 0.0), jnp.where(lane >= side, block, 0.0)], axis=0)


def dot_paired(a, block):
    return dot(a, paired(block))


def dot_paired_t(a, block):
    return lax.dot_general(
        a, paired(block), (((1,), (1,)), ((), ())), precision=highest, preferred_element_type=jnp.float32
    )


def halves(row, side):
    lane = lax.broadcasted_iota(jnp.int32, row.shape, 1)
    return [
        jnp.sum(jnp.where(lane < side, row, 0.0), axis=1, keepdims=True),
        jnp.sum(jnp.where(lane >= side, row, 0.0), axis=1, keepdims=True),
    ]


def eliminate_kernel(toa_devices, sums_ref, prior_ref, coupling_ref, power_ref, packed_ref, extra_ref):
    owned, height, columns = sums_ref.shape
    side = SIDE
    common = columns - prior_ref.shape[2]
    device = lax.axis_index("psr") * toa_devices + lax.axis_index("toa")
    lane_p = lax.broadcasted_iota(jnp.int32, (1, coupling_ref.shape[1]), 1)
    lane2 = lax.broadcasted_iota(jnp.int32, (1, 2 * side), 1)
    row2 = lax.broadcasted_iota(jnp.int32, (side, 2 * side), 0)
    col2 = lax.rem(lax.broadcasted_iota(jnp.int32, (side, 2 * side), 1), side)
    blocks = columns // side
    power = power_ref[...]
    power2 = jnp.concatenate([power, power], axis=1)
    for first in range(0, owned, 2):
        pair = (first, min(first + 1, owned - 1))

        def both(lo, hi, j):
            return jnp.concatenate([sums_ref[p, lo:hi, j * side : (j + 1) * side] for p in pair], axis=1)

        order = list(range(1, blocks)) + [0]
        a = {}
        for s, j in enumerate(order):
            for i in order[s:]:
                a[i, j] = both(i * side, (i + 1) * side, j)
            a["p", j] = both(columns, columns + 8, j)
            if j:
                own = jnp.concatenate([1.0 / prior_ref[p, :, (j - 1) * side : j * side] for p in pair], axis=1)
                a[j, j] = a[j, j] + jnp.where(row2 == col2, own, 0.0)
        logs = jnp.zeros((1, 2 * side), jnp.float32)
        quads = jnp.zeros((1, 2 * side), jnp.float32)
        for s, j in enumerate(order[:-1]):
            inverse, extra_logs = invert_pair(a[j, j], PANEL)
            logs = logs + extra_logs
            rest = order[s + 1 :]
            scaled = {i: dot_paired(a[i, j], inverse) for i in rest + ["p"]}
            quads = quads + scaled["p"][0:1] * a["p", j][0:1]
            for t, m in enumerate(rest):
                for i in rest[t:] + ["p"]:
                    a[i, m] = a[i, m] - dot_paired_t(scaled[i], a[m, j])
        owns = []
        for p in pair:
            at = device * owned + p
            owns.append(jnp.sum(jnp.where(lane_p == at, coupling_ref[pl.ds(at, 1), :], 0.0), axis=1, keepdims=True))
        own2 = jnp.where(lane2 < side, owns[0], owns[1])
        inverse, extra_logs = invert_pair(a[0, 0] + jnp.where(row2 == col2, own2 * power2, 0.0), PANEL)
        logs = halves(logs + extra_logs, side)
        quads = halves(quads, side)
        lane = lax.broadcasted_iota(jnp.int32, (1, 128 - common), 1)
        half = common // 2
        for h, p in enumerate(pair[: min(2, owned - first)]):
            tail = sums_ref[p, columns + 1 : columns + 2, :]
            energy = jnp.sum(tail[:, : columns // 2], axis=1, keepdims=True)
            count = jnp.sum(tail[:, columns // 2 :], axis=1, keepdims=True)
            mine = inverse[:, h * side : (h + 1) * side]
            packed_ref[p, 0:half, :] = jnp.concatenate([mine[:half], mine[half:]], axis=1)
            target = a["p", 0][0:1, h * side : (h + 1) * side]
            facts = jnp.where(lane == 0, logs[h] / columns, 0.0)
            facts = jnp.where(lane == 1, energy - quads[h], facts)
            facts = jnp.where(lane == 2, count, facts)
            line = jnp.concatenate([target, facts], axis=1)
            packed_ref[p, half : half + 8, :] = jnp.broadcast_to(line, (8, 128))
            extra_ref[p : p + 1, :] = line


def eliminate(sums, own_prior, coupling, power, toa_devices):
    owned, height, columns = sums.shape
    common = columns - own_prior.shape[1]
    return pl.pallas_call(
        functools.partial(eliminate_kernel, toa_devices),
        out_shape=(
            jax.ShapeDtypeStruct((owned, common // 2 + 8, 2 * common), jnp.float32),
            jax.ShapeDtypeStruct((owned, 2 * common), jnp.float32),
        ),
        name="eliminate",
    )(sums, own_prior[:, None, :], coupling, power)


def conjugate_kernel(packed_ref, coupling_ref, power_ref, out_ref, blocks_ref, w_ref):
    number = coupling_ref.shape[0]
    common = power_ref.shape[0]
    half = common // 2
    stride = half + 8

    def spread(k, carry):
        x = jnp.transpose(packed_ref[pl.ds(k, number, stride=stride), :])
        blocks_ref[k] = x[:common]
        blocks_ref[k + half] = x[common:]
        return carry

    lax.fori_loop(0, half, spread, 0)
    target = jnp.transpose(packed_ref[pl.ds(half, number, stride=stride), :])[:common]
    row = lax.broadcasted_iota(jnp.int32, (number, number), 0)
    col = lax.broadcasted_iota(jnp.int32, (number, number), 1)
    mixing = jnp.where(row == col, 0.0, coupling_ref[...])
    power = power_ref[...]

    def total(x):
        return jnp.sum(jnp.sum(x, axis=0, keepdims=True), axis=1, keepdims=True)

    def apply_blocks(v):
        w_ref[...] = v
        acc = jnp.zeros((common, number), jnp.float32)
        for k in range(common):
            acc = acc + blocks_ref[k] * w_ref[k : k + 1, :]
        return acc

    solution = jnp.zeros((common, number), jnp.float32)
    residual = target
    scaled = apply_blocks(residual)
    direction, block_direction = scaled, residual
    inner = total(residual * scaled)
    for iteration in range(ITERS):
        coupled = power * dot(direction, mixing)
        mapped = block_direction + coupled
        step = inner / total(direction * mapped)
        solution = solution + step * direction
        if iteration + 1 < ITERS:
            residual = residual - step * mapped
            scaled = scaled - step * (direction + apply_blocks(coupled))
            following = total(residual * scaled)
            ratio = following / inner
            direction = scaled + ratio * direction
            block_direction = residual + ratio * block_direction
            inner = following
    out_ref[...] = jnp.transpose(solution)


def conjugate(packed, coupling, power):
    number = coupling.shape[0]
    common = power.shape[0]
    return pl.pallas_call(
        conjugate_kernel,
        out_shape=jax.ShapeDtypeStruct((number, common), jnp.float32),
        scratch_shapes=[
            pltpu.VMEM((common, common, number), jnp.float32),
            pltpu.VMEM((common, number), jnp.float32),
        ],
        name="conjugate",
    )(packed.reshape(-1, packed.shape[-1]), coupling, power)


MESH = pl.DeviceIdType.MESH


def reduce_kernel(chips, partial_ref, out_ref, near_ref, sum_ref, far_ref, near_send, near_recv, far_send, far_recv):
    me = lax.axis_index("toa")
    core = lax.rem(me, 2)
    chip = me // 2
    other = 1 - core
    owned = out_ref.shape[0]
    barrier = pltpu.get_barrier_semaphore()
    pl.semaphore_signal(barrier, inc=1, device_id={"toa": chip * 2 + other}, device_id_type=MESH)
    for d in range(1, chips):
        target = lax.rem(chip + d, chips) * 2 + core
        pl.semaphore_signal(barrier, inc=1, device_id={"toa": target}, device_id_type=MESH)
    pl.semaphore_wait(barrier, chips)
    order = [d % chips for d in range(1, chips + 1)]
    near, far = {}, {}
    for d in order:
        owner = lax.rem(chip + d, chips) * 2 + other
        for i in range(owned):
            near[d, i] = pltpu.make_async_remote_copy(
                src_ref=partial_ref.at[owner * owned + i],
                dst_ref=near_ref.at[d * owned + i],
                send_sem=near_send.at[d * owned + i],
                recv_sem=near_recv.at[d * owned + i],
                device_id={"toa": chip * 2 + other},
                device_id_type=MESH,
            )
            near[d, i].start()
    for d in order:
        owner = lax.rem(chip + d, chips) * 2 + core
        for i in range(owned):
            at = d * owned + i
            near[d, i].wait_recv()
            both = partial_ref[owner * owned + i] + near_ref[at]
            if d == 0:
                out_ref[i] = both
                continue
            sum_ref[at - owned] = both
            far[d, i] = pltpu.make_async_remote_copy(
                src_ref=sum_ref.at[at - owned],
                dst_ref=far_ref.at[at - owned],
                send_sem=far_send.at[at - owned],
                recv_sem=far_recv.at[at - owned],
                device_id={"toa": owner},
                device_id_type=MESH,
            )
            far[d, i].start()
    for (d, i), copy in far.items():
        copy.wait_recv()
        out_ref[i] += far_ref[d * owned + i - owned]
    for copy in list(near.values()) + list(far.values()):
        copy.wait_send()


def reduce_owners(partial, toa_devices):
    pulsars, height, columns = partial.shape
    owned = pulsars // toa_devices
    chips = toa_devices // 2
    moved = owned * (chips - 1)
    block = (height, columns)
    return pl.pallas_call(
        functools.partial(reduce_kernel, chips),
        out_shape=jax.ShapeDtypeStruct((owned,) + block, jnp.float32),
        in_specs=[pl.BlockSpec(memory_space=pltpu.VMEM)],
        out_specs=pl.BlockSpec(memory_space=pltpu.VMEM),
        scratch_shapes=[
            pltpu.VMEM((owned * chips,) + block, jnp.float32),
            pltpu.VMEM((moved,) + block, jnp.float32),
            pltpu.VMEM((moved,) + block, jnp.float32),
            pltpu.SemaphoreType.DMA((owned * chips,)),
            pltpu.SemaphoreType.DMA((owned * chips,)),
            pltpu.SemaphoreType.DMA((moved,)),
            pltpu.SemaphoreType.DMA((moved,)),
        ],
        compiler_params=pltpu.CompilerParams(collective_id=0, has_side_effects=True),
        cost_estimate=pl.CostEstimate(flops=4 * pulsars * height * columns, bytes_accessed=40 * pulsars * height * columns, transcendentals=0),
        name="reduce_owners",
    )(partial)


def gather_kernel(groups, chips, mine_ref, out_ref, all_ref, psr_send, chip_send, core_send, recv):
    psr, me = lax.axis_index("psr"), lax.axis_index("toa")
    toa_devices = 2 * chips
    core = lax.rem(me, 2)
    chip = me // 2
    other = 1 - core
    partner = chip * 2 + other
    barrier = pltpu.get_barrier_semaphore()

    def greet(psr_to, toa_to):
        pl.semaphore_signal(barrier, inc=1, device_id={"psr": psr_to, "toa": toa_to}, device_id_type=MESH)

    greet(psr, partner)
    for d in range(1, chips):
        greet(psr, lax.rem(chip + d, chips) * 2 + core)
    for e in range(1, groups):
        greet(lax.rem(psr + e, groups), me)
    pl.semaphore_wait(barrier, chips + groups - 1)
    sent = []

    def block_of(e, toa):
        return lax.rem(psr + groups - e, groups) * toa_devices + toa

    def copy(source, block, sem, psr_to, toa_to):
        return pltpu.make_async_remote_copy(
            src_ref=source,
            dst_ref=all_ref.at[block],
            send_sem=sem,
            recv_sem=recv.at[block],
            device_id={"psr": psr_to, "toa": toa_to},
            device_id_type=MESH,
        )

    def send(source, block, sem, psr_to, toa_to):
        moving = copy(source, block, sem, psr_to, toa_to)
        moving.start()
        sent.append(moving)

    def arrived(block):
        copy(all_ref.at[block], block, core_send.at[0], psr, partner).wait_recv()

    own = psr * toa_devices + me
    for e in range(1, groups):
        send(mine_ref, own, psr_send.at[e - 1], lax.rem(psr + e, groups), me)
    for e in range(groups):
        block = block_of(e, me)
        if e:
            arrived(block)
        source = all_ref.at[block] if e else mine_ref
        for d in range(1, chips):
            send(source, block, chip_send.at[e * (chips - 1) + d - 1], psr, lax.rem(chip + d, chips) * 2 + core)
        send(source, block, core_send.at[e], psr, partner)
    for d in range(1, chips):
        for e in range(groups):
            block = block_of(e, lax.rem(chip + chips - d, chips) * 2 + core)
            arrived(block)
            send(all_ref.at[block], block, core_send.at[d * groups + e], psr, partner)
    all_ref[own] = mine_ref[...]
    for c in range(chips):
        for e in range(groups):
            arrived(block_of(e, c * 2 + other))
    for moving in sent:
        moving.wait_send()
    out_ref[...] = all_ref[...]


def gather_all(mine, groups, toa_devices):
    chips = toa_devices // 2
    devices = groups * toa_devices
    return pl.pallas_call(
        functools.partial(gather_kernel, groups, chips),
        out_shape=jax.ShapeDtypeStruct((devices,) + mine.shape, jnp.float32),
        in_specs=[pl.BlockSpec(memory_space=pltpu.VMEM)],
        out_specs=pl.BlockSpec(memory_space=pltpu.VMEM),
        scratch_shapes=[
            pltpu.VMEM((devices,) + mine.shape, jnp.float32),
            pltpu.SemaphoreType.DMA((groups - 1,)),
            pltpu.SemaphoreType.DMA((groups * (chips - 1),)),
            pltpu.SemaphoreType.DMA((groups * chips,)),
            pltpu.SemaphoreType.DMA((devices,)),
        ],
        compiler_params=pltpu.CompilerParams(collective_id=1, has_side_effects=True),
        name="gather_all",
    )(mine)


def body(design, noise_weight, residuals, slot_pulsar, slot_rows, own_prior, spectrum, directions):
    toa_devices = lax.axis_size("toa")
    owned = GROUP_PULSARS // toa_devices
    device = lax.axis_index("psr") * toa_devices + lax.axis_index("toa")
    partial = local_grams(design, noise_weight, residuals, slot_pulsar, slot_rows)
    sums = reduce_owners(partial, toa_devices)
    coupling = coupling_inverse(directions)
    power = 1.0 / jnp.repeat(spectrum, 2)
    packed, extra = eliminate(sums, own_prior, coupling, power[None, :], toa_devices)
    mine = packed.reshape(-1, packed.shape[-1])
    everything = gather_all(mine, lax.axis_size("psr"), toa_devices)
    whole = conjugate(everything, coupling, power[:, None])
    common = whole.shape[1]
    solution = lax.dynamic_slice_in_dim(whole, device * owned, owned, 0)
    chi_square = (extra[:, common + 1] - jnp.sum(extra[:, :common] * solution, axis=1)) / extra[:, common + 2]
    return (solution, extra[:, common], chi_square)


def solution(mesh):
    return jax.shard_map(
        body,
        mesh=mesh,
        in_specs=(
            P(("psr", "toa"), None, None),
            P(("psr", "toa"), None),
            P(("psr", "toa"), None),
            P(("psr", "toa")),
            P(("psr", "toa")),
            P(("psr", "toa"), None),
            P(),
            P(),
        ),
        out_specs=(P(("psr", "toa"), None), P(("psr", "toa")), P(("psr", "toa"))),
        check_vma=False,
    )
```

```python
import functools

import jax
import jax.numpy as jnp
from jax import lax
from jax.experimental import pallas as pl
from jax.experimental.pallas import tpu as pltpu
from jax.sharding import PartitionSpec as P

GROUP_PULSARS = 8
ITERS = 8
SIDE = 64
HALF = 32
LANES = 128
STEP_SLOTS = 16
PANEL = 16
highest = lax.Precision.HIGHEST
MESH = pl.DeviceIdType.MESH


def dot(a, b, precision=highest):
    return jnp.dot(a, b, precision=precision, preferred_element_type=jnp.float32)


def iota(shape, axis):
    return lax.broadcasted_iota(jnp.int32, shape, axis)


def gram_kernel(pulsar_ref, rows_ref, design_ref, weight_ref, residual_ref, out_ref, acc_ref):
    step = pl.program_id(0)
    toas, columns = design_ref.shape[1], design_ref.shape[2]
    half = columns // 2

    @pl.when(step == 0)
    def _():
        acc_ref[...] = jnp.zeros_like(acc_ref)

    lanes = iota((1, toas), 1)
    at_row = iota((8, half), 0)
    for j in range(STEP_SLOTS):
        slot = step * STEP_SLOTS + j
        p = pulsar_ref[slot]
        valid = lanes < rows_ref[slot]
        weight = jnp.where(valid, weight_ref[j : j + 1, :], 0.0)
        residual = residual_ref[j : j + 1, :].astype(jnp.float32)
        block = design_ref[j]
        across = jnp.transpose(block).astype(jnp.float32)
        weighted = (across * weight).astype(jnp.bfloat16)
        gram = jnp.dot(weighted, block, preferred_element_type=jnp.float32)
        spread = jnp.broadcast_to(residual, (8, toas)).astype(jnp.bfloat16)
        fitted = lax.dot_general(
            spread, weighted, (((1,), (1,)), ((), ())), preferred_element_type=jnp.float32
        )
        energy = weight * residual * residual
        count = jnp.where(valid, 1.0, 0.0)
        extra = jnp.where(at_row == 0, fitted[:, :half], jnp.where(at_row == 1, fitted[:, half:], 0.0))
        extra = jnp.where(at_row == 2, energy, jnp.where(at_row == 3, count, extra))
        acc_ref[p, 0:half, :] += gram[:half, :half]
        acc_ref[p, half:columns, :] += gram[:half, half:]
        acc_ref[p, columns : columns + half, :] += gram[half:, half:]
        acc_ref[p, columns + half : columns + half + 8, :] += extra

    @pl.when(step == pl.num_programs(0) - 1)
    def _():
        row, col = iota((half, half), 0), iota((half, half), 1)

        def pack(p, carry):
            low = acc_ref[p, columns : columns + half, :]
            out_ref[p, 0:half, :] = jnp.where(row >= col, acc_ref[p, 0:half, :], low)
            out_ref[p, half:columns, :] = acc_ref[p, half:columns, :]
            diag = jnp.sum(jnp.where(row == col, low, 0.0), axis=0, keepdims=True)
            tail = acc_ref[p, columns + half : columns + half + 8, :]
            out_ref[p, columns : columns + 8, :] = jnp.where(at_row == 4, diag, tail)
            return carry

        lax.fori_loop(0, GROUP_PULSARS, pack, 0)


def local_grams(design, noise_weight, residuals, slot_pulsar, slot_rows):
    slots, toas, columns = design.shape
    half = columns // 2
    return pl.pallas_call(
        gram_kernel,
        grid_spec=pltpu.PrefetchScalarGridSpec(
            num_scalar_prefetch=2,
            grid=(slots // STEP_SLOTS,),
            in_specs=[
                pl.BlockSpec((STEP_SLOTS, toas, columns), lambda i, *_: (i, 0, 0)),
                pl.BlockSpec((STEP_SLOTS, toas), lambda i, *_: (i, 0)),
                pl.BlockSpec((STEP_SLOTS, toas), lambda i, *_: (i, 0)),
            ],
            out_specs=pl.BlockSpec((GROUP_PULSARS, columns + 8, half), lambda i, *_: (0, 0, 0)),
            scratch_shapes=[pltpu.VMEM((GROUP_PULSARS, columns + half + 8, half), jnp.float32)],
        ),
        out_shape=jax.ShapeDtypeStruct((GROUP_PULSARS, columns + 8, half), jnp.float32),
        name="gram",
    )(slot_pulsar, slot_rows, design, noise_weight, residuals)


def invert_pair(x, width):
    side, lanes = x.shape
    within = lax.rem(iota((1, lanes), 1), side)
    half = iota((side, lanes), 1)
    half = half - lax.rem(half, side)
    sub = iota((width, lanes), 0)
    pivots = jnp.ones((1, lanes), jnp.float32)
    for lo in range(0, side, width):
        hi = lo + width
        columns = [jnp.take_along_axis(x, half + (lo + k), axis=1) for k in range(width)]
        rows = x[lo:hi]
        inner = [c[lo:hi] for c in columns]
        for k in range(width):
            here = within == lo + k
            pivot = inner[k][k : k + 1]
            inverse = 1.0 / pivot
            pivots = jnp.where(here, pivot, pivots)
            row = jnp.where(here, 1.0, rows[k : k + 1]) * inverse
            at = sub == k
            rows = jnp.where(at, row, jnp.where(here, 0.0, rows) - inner[k] * row)
            for j in range(k + 1, width):
                scaled = inner[j][k : k + 1] * inverse
                inner[j] = jnp.where(at, scaled, inner[j] - inner[k] * scaled)
        inside = (within >= lo) & (within < hi)
        parts = []
        for begin in range(0, side, width):
            if begin == lo:
                parts.append(rows)
                continue
            acc = jnp.where(inside, 0.0, x[begin : begin + width])
            for k in range(width):
                acc = acc - columns[k][begin : begin + width] * rows[k : k + 1]
            parts.append(acc)
        x = jnp.concatenate(parts, axis=0)
    return x, jnp.log(pivots)


def coupling_inverse(directions, owned):
    number = directions.shape[1]
    row, col = iota((number, number), 0), iota((number, number), 1)
    if owned > 1:
        devices = number // owned
        source = lax.rem(col, devices) * owned + col // devices
        directions = dot(directions, jnp.where(row == source, 1.0, 0.0))
    cosines = lax.dot_general(
        directions, directions, (((0,), (0,)), ((), ())), precision=highest, preferred_element_type=jnp.float32
    )
    cosines = jnp.clip(cosines, -1.0, 1.0)
    spread = jnp.where(row == col, 1.0, 0.5 * (1.0 - cosines))
    curve = 1.5 * spread * jnp.log(spread) - 0.25 * spread + 0.5
    x = jnp.where(row == col, 1.0, curve)
    if number == SIDE:
        return invert_pair(jnp.concatenate([x, x], axis=1), PANEL)[0]
    tiles = number // SIDE
    for b in range(tiles):
        lo, hi = b * SIDE, (b + 1) * SIDE
        block = x[lo:hi, lo:hi]
        inverse = invert_pair(jnp.concatenate([block, block], axis=1), PANEL)[0][:, :SIDE]
        across = dot(inverse, x[lo:hi, :])
        down = x[:, lo:hi]
        inside_row = (row >= lo) & (row < hi)
        inside_col = (col >= lo) & (col < hi)
        updated = x - dot(down, across)
        placed = -dot(down, inverse)
        updated = jnp.where(inside_col, jnp.concatenate([placed] * tiles, axis=1), updated)
        fixed = jnp.where(
            inside_col,
            jnp.concatenate([jnp.concatenate([inverse] * tiles, axis=1)] * tiles, axis=0),
            jnp.concatenate([across] * tiles, axis=0),
        )
        x = jnp.where(inside_row, fixed, updated)
    return x


def reduce_kernel(
    chips, partial_ref, directions_ref, out_ref, coupling_ref, near_ref, sum_ref, far_ref, pad_ref,
    near_send, near_recv, far_send, far_recv
):
    me = lax.axis_index("toa")
    core = lax.rem(me, 2)
    chip = me // 2
    other = 1 - core
    owned = out_ref.shape[0]
    barrier = pltpu.get_barrier_semaphore()
    pl.semaphore_signal(barrier, inc=1, device_id={"toa": chip * 2 + other}, device_id_type=MESH)
    for d in range(1, chips):
        target = lax.rem(chip + d, chips) * 2 + core
        pl.semaphore_signal(barrier, inc=1, device_id={"toa": target}, device_id_type=MESH)
    pl.semaphore_wait(barrier, chips)
    order = [d % chips for d in range(1, chips + 1)]
    near, far = {}, {}
    for d in order:
        owner = lax.rem(chip + d, chips) * 2 + other
        for i in range(owned):
            near[d, i] = pltpu.make_async_remote_copy(
                src_ref=partial_ref.at[owner * owned + i],
                dst_ref=near_ref.at[d * owned + i],
                send_sem=near_send.at[d * owned + i],
                recv_sem=near_recv.at[d * owned + i],
                device_id={"toa": chip * 2 + other},
                device_id_type=MESH,
            )
            near[d, i].start()
    for d in order:
        owner = lax.rem(chip + d, chips) * 2 + core
        for i in range(owned):
            at = d * owned + i
            near[d, i].wait_recv()
            both = partial_ref[owner * owned + i] + near_ref[at]
            if d == 0:
                out_ref[i] = both
                continue
            sum_ref[at - owned] = both
            far[d, i] = pltpu.make_async_remote_copy(
                src_ref=sum_ref.at[at - owned],
                dst_ref=far_ref.at[at - owned],
                send_sem=far_send.at[at - owned],
                recv_sem=far_recv.at[at - owned],
                device_id={"toa": owner},
                device_id_type=MESH,
            )
            far[d, i].start()
    pad_ref[...] = jnp.zeros_like(pad_ref)
    pad_ref[0 : directions_ref.shape[0], :] = directions_ref[...]
    coupling_ref[...] = coupling_inverse(pad_ref[...], owned)
    for (d, i), copy in far.items():
        copy.wait_recv()
        out_ref[i] += far_ref[d * owned + i - owned]
    for copy in list(near.values()) + list(far.values()):
        copy.wait_send()


def reduce_owners(partial, directions, toa_devices):
    pulsars, height, lanes = partial.shape
    number = directions.shape[1]
    owned = pulsars // toa_devices
    chips = toa_devices // 2
    moved = owned * (chips - 1)
    block = (height, lanes)
    vmem = pl.BlockSpec(memory_space=pltpu.VMEM)
    return pl.pallas_call(
        functools.partial(reduce_kernel, chips),
        out_shape=(
            jax.ShapeDtypeStruct((owned,) + block, jnp.float32),
            jax.ShapeDtypeStruct((number, LANES), jnp.float32),
        ),
        in_specs=[vmem, vmem],
        out_specs=(vmem, vmem),
        scratch_shapes=[
            pltpu.VMEM((owned * chips,) + block, jnp.float32),
            pltpu.VMEM((moved,) + block, jnp.float32),
            pltpu.VMEM((moved,) + block, jnp.float32),
            pltpu.VMEM((8, number), jnp.float32),
            pltpu.SemaphoreType.DMA((owned * chips,)),
            pltpu.SemaphoreType.DMA((owned * chips,)),
            pltpu.SemaphoreType.DMA((moved,)),
            pltpu.SemaphoreType.DMA((moved,)),
        ],
        compiler_params=pltpu.CompilerParams(collective_id=0, has_side_effects=True),
        cost_estimate=pl.CostEstimate(flops=4 * pulsars * height * lanes, bytes_accessed=40 * pulsars * height * lanes, transcendentals=0),
        name="reduce_owners",
    )(partial, directions)


def paired(block):
    side, lanes = block.shape
    left = iota((side, lanes), 1) < side
    return jnp.concatenate([jnp.where(left, block, 0.0), jnp.where(left, 0.0, block)], axis=0)


def dot_paired(a, block):
    return dot(a, paired(block))


def dot_paired_t(a, block):
    return lax.dot_general(
        a, paired(block), (((1,), (1,)), ((), ())), precision=highest, preferred_element_type=jnp.float32
    )


def halves(row, side):
    left = iota(row.shape, 1) < side
    return [
        jnp.sum(jnp.where(left, row, 0.0), axis=1, keepdims=True),
        jnp.sum(jnp.where(left, 0.0, row), axis=1, keepdims=True),
    ]


def payload_rows(owned):
    return -(-17 * owned // 8) * 8


def eliminate_kernel(devices, toa_devices, sums_ref, prior_ref, coupling_ref, spectrum_ref, packed_ref, facts_ref):
    owned, height, lanes = sums_ref.shape
    side = SIDE
    columns = height - 8
    blocks = columns // side
    device = lax.axis_index("psr") * toa_devices + lax.axis_index("toa")
    lane = iota((1, lanes), 1)
    left = lane < side
    row2 = iota((side, lanes), 0)
    col2 = lax.rem(iota((side, lanes), 1), side)
    freqs = spectrum_ref.shape[1]
    pick = jnp.where(iota((freqs, lanes), 0) == lax.rem(iota((freqs, lanes), 1), side) // 2, 1.0, 0.0)
    power2 = dot(jnp.broadcast_to(1.0 / spectrum_ref[...], (8, freqs)), pick)[0:1]
    row1, col1 = iota((lanes, lanes), 0), iota((lanes, lanes), 1)
    packed_ref[...] = jnp.zeros_like(packed_ref)
    for first in range(0, owned, 2):
        pair = (first, min(first + 1, owned - 1))
        whole = []
        for p in pair:
            mixed = sums_ref[p, 0:lanes, :]
            turned = jnp.transpose(mixed)
            diag = sums_ref[p, columns + 4 : columns + 5, :]
            top = jnp.where(row1 >= col1, mixed, turned)
            low = jnp.where(row1 < col1, mixed, jnp.where(row1 == col1, diag, turned))
            whole.append({(0, 0): top, (0, 1): sums_ref[p, lanes : 2 * lanes, :], (1, 1): low})

        def join(parts, j):
            if j % 2 == 0:
                return jnp.where(left, parts[0], pltpu.roll(parts[1], side, 1))
            return jnp.where(left, pltpu.roll(parts[0], side, 1), parts[1])

        def both(i, j):
            lo = (i % 2) * side
            return join([w[i // 2, j // 2][lo : lo + side] for w in whole], j)

        order = list(range(blocks - 1, -1, -1))
        a = {}
        for s, j in enumerate(order):
            for i in order[s:]:
                a[i, j] = both(i, j)
            at = columns + j // 2
            a["p", j] = join([jnp.broadcast_to(sums_ref[p, at : at + 1, :], (8, lanes)) for p in pair], j)
            if j:
                own = jnp.concatenate([1.0 / prior_ref[p : p + 1, (j - 1) * side : j * side] for p in pair], axis=1)
                a[j, j] = a[j, j] + jnp.where(row2 == col2, own, 0.0)
        logs = jnp.zeros((1, lanes), jnp.float32)
        quads = jnp.zeros((1, lanes), jnp.float32)
        for s, j in enumerate(order[:-1]):
            inverse, extra_logs = invert_pair(a[j, j], PANEL)
            logs = logs + extra_logs
            rest = order[s + 1 :]
            scaled = {i: dot_paired(a[i, j], inverse) for i in rest + ["p"]}
            quads = quads + scaled["p"][0:1] * a["p", j][0:1]
            for t, m in enumerate(rest):
                for i in rest[t:] + ["p"]:
                    a[i, m] = a[i, m] - dot_paired_t(scaled[i], a[m, j])
        owns = []
        for h, p in enumerate(pair):
            at = (p * devices) + device
            line = coupling_ref[pl.ds(at, 1), :]
            here = lane == at
            owns.append(jnp.sum(jnp.where(here, line, 0.0), axis=1, keepdims=True))
        own2 = jnp.where(left, owns[0], owns[1])
        x, extra_logs = invert_pair(a[0, 0] + jnp.where(row2 == col2, own2 * power2, 0.0), PANEL)
        logs = halves(logs + extra_logs, side)
        quads = halves(quads, side)
        row3, col3 = row2[:HALF], col2[:HALF]
        bottom = pltpu.roll(x[HALF:], lanes - HALF, 1)
        packed = jnp.where((col3 < HALF) & (row3 < col3), bottom, x[:HALF])
        diag = jnp.sum(jnp.where(row3 + HALF == col3, x[HALF:], 0.0), axis=0, keepdims=True)
        target = a["p", 0][0:1]
        turned = pltpu.roll(packed, side, 1)
        quarter = HALF // 2
        for h, p in enumerate(pair[: min(2, owned - first)]):
            tail = sums_ref[p, columns + 2 : columns + 4, :]
            energy = jnp.sum(tail[0:1], axis=1, keepdims=True)
            count = jnp.sum(tail[1:2], axis=1, keepdims=True)
            if h == 0:
                mine = jnp.where(left, packed[:quarter], turned[quarter:])
                line = jnp.where(left, target, pltpu.roll(diag, HALF, 1))
            else:
                mine = jnp.where(left, turned[:quarter], packed[quarter:])
                line = jnp.where(left, pltpu.roll(target, side, 1), pltpu.roll(diag, lanes - HALF, 1))
            packed_ref[p * quarter : (p + 1) * quarter, :] = mine
            at = owned * quarter + p
            packed_ref[at : at + 1, :] = line
            facts = jnp.where(lane == side, logs[h] / columns, line)
            facts = jnp.where(lane == side + 1, energy - quads[h], facts)
            facts = jnp.where(lane == side + 2, count, facts)
            facts_ref[p : p + 1, :] = facts


def eliminate(sums, own_prior, coupling, spectrum, devices, toa_devices):
    owned, height, lanes = sums.shape
    return pl.pallas_call(
        functools.partial(eliminate_kernel, devices, toa_devices),
        out_shape=(
            jax.ShapeDtypeStruct((payload_rows(owned), lanes), jnp.float32),
            jax.ShapeDtypeStruct((owned, lanes), jnp.float32),
        ),
        name="eliminate",
    )(sums, own_prior, coupling, spectrum)


def total(x):
    return jnp.sum(jnp.sum(x, axis=0, keepdims=True), axis=1, keepdims=True)


def split(x):
    high = x.astype(jnp.bfloat16)
    return high, (x - high.astype(jnp.float32)).astype(jnp.bfloat16)


def conjugate(all_ref, coupling_ref, spectrum_ref, turned_ref, blocks_ref, w_ref, devices, owned):
    number = devices * owned
    rows = payload_rows(owned)
    quarter = HALF // 2
    fold = LANES // number

    def across(at):
        parts = [all_ref[pl.ds(begin, devices, stride=rows), :] for begin in at]
        return jnp.transpose(jnp.concatenate(parts * fold, axis=0))

    def turn(r, carry):
        x = across([h * quarter + r for h in range(owned)])
        turned_ref[pl.ds(pl.multiple_of(r * SIDE, SIDE), SIDE), :] = x[:SIDE]
        turned_ref[pl.ds(pl.multiple_of((r + quarter) * SIDE, SIDE), SIDE), :] = x[SIDE:]
        return carry

    for r in range(quarter):
        turn(r, 0)
    x = across([owned * quarter + h for h in range(owned)])
    target, diag = x[:SIDE], x[SIDE : SIDE + HALF]
    left = iota((HALF, LANES), 1) < SIDE
    sub = iota((HALF, LANES), 0)

    for r in range(HALF):
        mine = turned_ref[r * SIDE : r * SIDE + HALF, :]
        beside = turned_ref[r * SIDE + HALF : (r + 1) * SIDE, :]
        mirror = turned_ref[pl.ds(r, HALF, stride=SIDE), :]
        below = turned_ref[pl.ds(r + HALF, HALF, stride=SIDE), :]
        first = jnp.where(sub <= r, mine, mirror)
        last = jnp.where(sub > r, mine, jnp.where(sub == r, diag, mirror))
        if fold == 2:
            blocks_ref[r, 0:HALF, :] = jnp.where(left, first, below)
            blocks_ref[r, HALF:SIDE, :] = jnp.where(left, beside, last)
        else:
            blocks_ref[r, 0:HALF, :] = first
            blocks_ref[r, HALF:SIDE, :] = beside
            blocks_ref[r + HALF, 0:HALF, :] = below
            blocks_ref[r + HALF, HALF:SIDE, :] = last

    coupling = coupling_ref[...]
    row, col = iota(coupling.shape, 0), iota(coupling.shape, 1)
    high, low = split(jnp.where(row == lax.rem(col, number), 0.0, coupling))
    freqs = spectrum_ref.shape[1]
    place = jnp.where(iota((SIDE, freqs), 0) // 2 == iota((SIDE, freqs), 1), 1.0 / spectrum_ref[...], 0.0)
    power = dot(place, jnp.ones((freqs, LANES), jnp.float32))
    wide = iota((SIDE, LANES), 1) < SIDE

    def mix(v):
        top, rest = split(v)
        if fold == 2:
            x = jnp.where(wide, top.astype(jnp.float32), rest.astype(jnp.float32)).astype(jnp.bfloat16)
            out = jnp.dot(
                jnp.concatenate([x, x], axis=1),
                jnp.concatenate([high, high, low, low], axis=0),
                preferred_element_type=jnp.float32,
            )
        else:
            x = jnp.concatenate([top, rest], axis=1)
            out = jnp.dot(x, jnp.concatenate([high, high], axis=0), preferred_element_type=jnp.float32)
            out = out + jnp.dot(x, jnp.concatenate([low, low], axis=0), preferred_element_type=jnp.float32)
        return power * out

    def apply_blocks(v):
        if fold == 2:
            w_ref[0:HALF, :] = jnp.where(left, v[:HALF], v[HALF:])
        else:
            w_ref[...] = v
        acc = jnp.zeros((SIDE, LANES), jnp.float32)
        for k in range(SIDE // fold):
            acc = acc + blocks_ref[k] * w_ref[k : k + 1, :]
        return acc + pltpu.roll(acc, SIDE, 1) if fold == 2 else acc

    residual = target
    scaled = apply_blocks(residual)
    inner = total(residual * scaled)
    mixed = mix(scaled)
    solved = apply_blocks(mixed)
    direction, block_direction = scaled, residual
    solution = jnp.zeros((SIDE, LANES), jnp.float32)
    for iteration in range(ITERS):
        mapped = block_direction + mixed
        step = inner / total(direction * mapped)
        solution = solution + step * direction
        if iteration + 1 == ITERS:
            break
        residual = residual - step * mapped
        scaled = scaled - step * (direction + solved)
        following = total(residual * scaled)
        ratio = following / inner
        fresh = mix(scaled)
        if iteration + 2 < ITERS:
            solved = apply_blocks(fresh) + ratio * solved
        mixed = fresh + ratio * mixed
        direction = scaled + ratio * direction
        block_direction = residual + ratio * block_direction
        inner = following
    return solution


def gather_kernel(
    groups, chips, mine_ref, coupling_ref, spectrum_ref, facts_ref, out_ref, logs_ref, chi_ref,
    all_ref, turned_ref, blocks_ref, w_ref, final_ref, psr_send, chip_send, core_send, recv
):
    psr, me = lax.axis_index("psr"), lax.axis_index("toa")
    toa_devices = 2 * chips
    devices = groups * toa_devices
    core = lax.rem(me, 2)
    chip = me // 2
    other = 1 - core
    partner = chip * 2 + other
    rows = mine_ref.shape[0]
    owned = out_ref.shape[0]
    barrier = pltpu.get_barrier_semaphore()

    def greet(psr_to, toa_to):
        pl.semaphore_signal(barrier, inc=1, device_id={"psr": psr_to, "toa": toa_to}, device_id_type=MESH)

    greet(psr, partner)
    for d in range(1, chips):
        greet(psr, lax.rem(chip + d, chips) * 2 + core)
    for e in range(1, groups):
        greet(lax.rem(psr + e, groups), me)
    pl.semaphore_wait(barrier, chips + groups - 1)
    sent = []

    def block_of(e, toa):
        return lax.rem(psr + groups - e, groups) * toa_devices + toa

    def slot(block):
        return all_ref.at[pl.ds(pl.multiple_of(block * rows, 8), rows)]

    def copy(source, block, sem, psr_to, toa_to):
        return pltpu.make_async_remote_copy(
            src_ref=source,
            dst_ref=slot(block),
            send_sem=sem,
            recv_sem=recv.at[block],
            device_id={"psr": psr_to, "toa": toa_to},
            device_id_type=MESH,
        )

    def send(source, block, sem, psr_to, toa_to):
        moving = copy(source, block, sem, psr_to, toa_to)
        moving.start()
        sent.append(moving)

    def arrived(block):
        copy(slot(block), block, core_send.at[0], psr, partner).wait_recv()

    own = psr * toa_devices + me
    for e in range(1, groups):
        send(mine_ref, own, psr_send.at[e - 1], lax.rem(psr + e, groups), me)
    for e in range(groups):
        block = block_of(e, me)
        if e:
            arrived(block)
        source = slot(block) if e else mine_ref
        for d in range(1, chips):
            send(source, block, chip_send.at[e * (chips - 1) + d - 1], psr, lax.rem(chip + d, chips) * 2 + core)
        send(source, block, core_send.at[e], psr, partner)
    for d in range(1, chips):
        for e in range(groups):
            block = block_of(e, lax.rem(chip + chips - d, chips) * 2 + core)
            arrived(block)
            send(slot(block), block, core_send.at[d * groups + e], psr, partner)
    all_ref[pl.ds(pl.multiple_of(own * rows, 8), rows), :] = mine_ref[...]
    for c in range(chips):
        for e in range(groups):
            arrived(block_of(e, c * 2 + other))
    for moving in sent:
        moving.wait_send()
    solution = conjugate(all_ref, coupling_ref, spectrum_ref, turned_ref, blocks_ref, w_ref, devices, owned)
    final_ref[...] = jnp.transpose(jnp.concatenate([solution, solution], axis=0))
    lane = iota((1, LANES), 1)
    for h in range(owned):
        mine = final_ref[pl.ds(h * devices + own, 1), :]
        out_ref[h : h + 1, :] = mine[:, :SIDE]
        facts = facts_ref[h : h + 1, :]
        fit = jnp.sum(jnp.where(lane < SIDE, facts * mine, 0.0), axis=1, keepdims=True)

        def at(k):
            return jnp.sum(jnp.where(lane == SIDE + k, facts, 0.0), axis=1, keepdims=True)

        logs_ref[h : h + 1, :] = jnp.broadcast_to(at(0), (1, LANES))
        chi_ref[h : h + 1, :] = jnp.broadcast_to((at(1) - fit) / at(2), (1, LANES))


def finish(mine, coupling, spectrum, facts, groups, toa_devices):
    chips = toa_devices // 2
    devices = groups * toa_devices
    rows = mine.shape[0]
    owned = facts.shape[0]
    fold = LANES // (devices * owned)
    vmem = pl.BlockSpec(memory_space=pltpu.VMEM)
    return pl.pallas_call(
        functools.partial(gather_kernel, groups, chips),
        out_shape=(
            jax.ShapeDtypeStruct((owned, SIDE), jnp.float32),
            jax.ShapeDtypeStruct((owned, LANES), jnp.float32),
            jax.ShapeDtypeStruct((owned, LANES), jnp.float32),
        ),
        in_specs=[vmem] * 4,
        out_specs=(vmem,) * 3,
        scratch_shapes=[
            pltpu.VMEM((devices * rows, LANES), jnp.float32),
            pltpu.VMEM((HALF * SIDE, LANES), jnp.float32),
            pltpu.VMEM((SIDE // fold, SIDE, LANES), jnp.float32),
            pltpu.VMEM((SIDE, LANES), jnp.float32),
            pltpu.VMEM((LANES, LANES), jnp.float32),
            pltpu.SemaphoreType.DMA((groups - 1,)),
            pltpu.SemaphoreType.DMA((groups * (chips - 1),)),
            pltpu.SemaphoreType.DMA((groups * chips,)),
            pltpu.SemaphoreType.DMA((devices,)),
        ],
        compiler_params=pltpu.CompilerParams(collective_id=1, has_side_effects=True),
        name="finish",
    )(mine, coupling, spectrum, facts)


def body(design, noise_weight, residuals, slot_pulsar, slot_rows, own_prior, spectrum, directions):
    groups, toa_devices = lax.axis_size("psr"), lax.axis_size("toa")
    partial = local_grams(design, noise_weight, residuals, slot_pulsar, slot_rows)
    sums, coupling = reduce_owners(partial, directions, toa_devices)
    spectrum = spectrum[None, :]
    packed, facts = eliminate(sums, own_prior, coupling, spectrum, groups * toa_devices, toa_devices)
    coeffs, log_dets, chi_square = finish(packed, coupling, spectrum, facts, groups, toa_devices)
    return (coeffs, log_dets[:, 0], chi_square[:, 0])


def solution(mesh):
    return jax.shard_map(
        body,
        mesh=mesh,
        in_specs=(
            P(("psr", "toa"), None, None),
            P(("psr", "toa"), None),
            P(("psr", "toa"), None),
            P(("psr", "toa")),
            P(("psr", "toa")),
            P(("psr", "toa"), None),
            P(),
            P(),
        ),
        out_specs=(P(("psr", "toa"), None), P(("psr", "toa")), P(("psr", "toa"))),
        check_vma=False,
    )
```

```python
import functools

import jax
import jax.numpy as jnp
from jax import lax
from jax.experimental import pallas as pl
from jax.experimental.pallas import tpu as pltpu
from jax.sharding import PartitionSpec as P

GROUP_PULSARS = 8
ITERS = 8
SIDE = 64
HALF = 32
LANES = 128
STEP_SLOTS = 16
PANEL = 16
highest = lax.Precision.HIGHEST
MESH = pl.DeviceIdType.MESH


def dot(a, b, precision=highest):
    return jnp.dot(a, b, precision=precision, preferred_element_type=jnp.float32)


def iota(shape, axis):
    return lax.broadcasted_iota(jnp.int32, shape, axis)


def gram_kernel(pulsar_ref, rows_ref, design_ref, weight_ref, residual_ref, out_ref, acc_ref):
    step = pl.program_id(0)
    toas, columns = design_ref.shape[1], design_ref.shape[2]
    half = columns // 2

    @pl.when(step == 0)
    def _():
        acc_ref[...] = jnp.zeros_like(acc_ref)

    lanes = iota((1, toas), 1)
    at_row = iota((8, half), 0)
    for j in range(STEP_SLOTS):
        slot = step * STEP_SLOTS + j
        p = pulsar_ref[slot]
        valid = lanes < rows_ref[slot]
        weight = jnp.where(valid, weight_ref[j : j + 1, :], 0.0)
        residual = residual_ref[j : j + 1, :].astype(jnp.float32)
        block = design_ref[j]
        across = jnp.transpose(block).astype(jnp.float32)
        weighted = (across * weight).astype(jnp.bfloat16)
        gram = jnp.dot(weighted, block, preferred_element_type=jnp.float32)
        spread = jnp.broadcast_to(residual, (8, toas)).astype(jnp.bfloat16)
        fitted = lax.dot_general(
            spread, weighted, (((1,), (1,)), ((), ())), preferred_element_type=jnp.float32
        )
        energy = weight * residual * residual
        count = jnp.where(valid, 1.0, 0.0)
        extra = jnp.where(at_row == 0, fitted[:, :half], jnp.where(at_row == 1, fitted[:, half:], 0.0))
        extra = jnp.where(at_row == 2, energy, jnp.where(at_row == 3, count, extra))
        acc_ref[p, 0:half, :] += gram[:half, :half]
        acc_ref[p, half:columns, :] += gram[:half, half:]
        acc_ref[p, columns : columns + half, :] += gram[half:, half:]
        acc_ref[p, columns + half : columns + half + 8, :] += extra

    @pl.when(step == pl.num_programs(0) - 1)
    def _():
        row, col = iota((half, half), 0), iota((half, half), 1)

        def pack(p, carry):
            low = acc_ref[p, columns : columns + half, :]
            out_ref[p, 0:half, :] = jnp.where(row >= col, acc_ref[p, 0:half, :], low)
            out_ref[p, half:columns, :] = acc_ref[p, half:columns, :]
            diag = jnp.sum(jnp.where(row == col, low, 0.0), axis=0, keepdims=True)
            tail = acc_ref[p, columns + half : columns + half + 8, :]
            out_ref[p, columns : columns + 8, :] = jnp.where(at_row == 4, diag, tail)
            return carry

        lax.fori_loop(0, GROUP_PULSARS, pack, 0)


def local_grams(design, noise_weight, residuals, slot_pulsar, slot_rows):
    slots, toas, columns = design.shape
    half = columns // 2
    return pl.pallas_call(
        gram_kernel,
        grid_spec=pltpu.PrefetchScalarGridSpec(
            num_scalar_prefetch=2,
            grid=(slots // STEP_SLOTS,),
            in_specs=[
                pl.BlockSpec((STEP_SLOTS, toas, columns), lambda i, *_: (i, 0, 0)),
                pl.BlockSpec((STEP_SLOTS, toas), lambda i, *_: (i, 0)),
                pl.BlockSpec((STEP_SLOTS, toas), lambda i, *_: (i, 0)),
            ],
            out_specs=pl.BlockSpec((GROUP_PULSARS, columns + 8, half), lambda i, *_: (0, 0, 0)),
            scratch_shapes=[pltpu.VMEM((GROUP_PULSARS, columns + half + 8, half), jnp.float32)],
        ),
        out_shape=jax.ShapeDtypeStruct((GROUP_PULSARS, columns + 8, half), jnp.float32),
        name="gram",
    )(slot_pulsar, slot_rows, design, noise_weight, residuals)


def invert_pair(x, width):
    side, lanes = x.shape
    within = lax.rem(iota((1, lanes), 1), side)
    half = iota((side, lanes), 1)
    half = half - lax.rem(half, side)
    sub = iota((width, lanes), 0)
    pivots = jnp.ones((1, lanes), jnp.float32)
    for lo in range(0, side, width):
        hi = lo + width
        columns = [jnp.take_along_axis(x, half + (lo + k), axis=1) for k in range(width)]
        rows = x[lo:hi]
        inner = [c[lo:hi] for c in columns]
        for k in range(width):
            here = within == lo + k
            pivot = inner[k][k : k + 1]
            inverse = 1.0 / pivot
            pivots = jnp.where(here, pivot, pivots)
            row = jnp.where(here, 1.0, rows[k : k + 1]) * inverse
            at = sub == k
            rows = jnp.where(at, row, jnp.where(here, 0.0, rows) - inner[k] * row)
            for j in range(k + 1, width):
                scaled = inner[j][k : k + 1] * inverse
                inner[j] = jnp.where(at, scaled, inner[j] - inner[k] * scaled)
        inside = (within >= lo) & (within < hi)
        parts = []
        for begin in range(0, side, width):
            if begin == lo:
                parts.append(rows)
                continue
            acc = jnp.where(inside, 0.0, x[begin : begin + width])
            for k in range(width):
                acc = acc - columns[k][begin : begin + width] * rows[k : k + 1]
            parts.append(acc)
        x = jnp.concatenate(parts, axis=0)
    return x, jnp.log(pivots)


def coupling_inverse(directions, owned):
    number = directions.shape[1]
    row, col = iota((number, number), 0), iota((number, number), 1)
    if owned > 1:
        devices = number // owned
        source = lax.rem(col, devices) * owned + col // devices
        directions = dot(directions, jnp.where(row == source, 1.0, 0.0))
    cosines = lax.dot_general(
        directions, directions, (((0,), (0,)), ((), ())), precision=highest, preferred_element_type=jnp.float32
    )
    cosines = jnp.clip(cosines, -1.0, 1.0)
    spread = jnp.where(row == col, 1.0, 0.5 * (1.0 - cosines))
    curve = 1.5 * spread * jnp.log(spread) - 0.25 * spread + 0.5
    x = jnp.where(row == col, 1.0, curve)
    if number == SIDE:
        return invert_pair(jnp.concatenate([x, x], axis=1), PANEL)[0]
    tiles = number // SIDE
    for b in range(tiles):
        lo, hi = b * SIDE, (b + 1) * SIDE
        block = x[lo:hi, lo:hi]
        inverse = invert_pair(jnp.concatenate([block, block], axis=1), PANEL)[0][:, :SIDE]
        across = dot(inverse, x[lo:hi, :])
        down = x[:, lo:hi]
        inside_row = (row >= lo) & (row < hi)
        inside_col = (col >= lo) & (col < hi)
        updated = x - dot(down, across)
        placed = -dot(down, inverse)
        updated = jnp.where(inside_col, jnp.concatenate([placed] * tiles, axis=1), updated)
        fixed = jnp.where(
            inside_col,
            jnp.concatenate([jnp.concatenate([inverse] * tiles, axis=1)] * tiles, axis=0),
            jnp.concatenate([across] * tiles, axis=0),
        )
        x = jnp.where(inside_row, fixed, updated)
    return x


def reduce_kernel(
    chips, partial_ref, directions_ref, out_ref, coupling_ref, near_ref, sum_ref, far_ref, pad_ref,
    near_send, near_recv, far_send, far_recv
):
    me = lax.axis_index("toa")
    core = lax.rem(me, 2)
    chip = me // 2
    other = 1 - core
    owned = out_ref.shape[0]
    barrier = pltpu.get_barrier_semaphore()
    pl.semaphore_signal(barrier, inc=1, device_id={"toa": chip * 2 + other}, device_id_type=MESH)
    for d in range(1, chips):
        target = lax.rem(chip + d, chips) * 2 + core
        pl.semaphore_signal(barrier, inc=1, device_id={"toa": target}, device_id_type=MESH)
    pl.semaphore_wait(barrier, chips)
    order = [d % chips for d in range(1, chips + 1)]
    near, far = {}, {}
    for d in order:
        owner = lax.rem(chip + d, chips) * 2 + other
        for i in range(owned):
            near[d, i] = pltpu.make_async_remote_copy(
                src_ref=partial_ref.at[owner * owned + i],
                dst_ref=near_ref.at[d * owned + i],
                send_sem=near_send.at[d * owned + i],
                recv_sem=near_recv.at[d * owned + i],
                device_id={"toa": chip * 2 + other},
                device_id_type=MESH,
            )
            near[d, i].start()
    for d in order:
        owner = lax.rem(chip + d, chips) * 2 + core
        for i in range(owned):
            at = d * owned + i
            near[d, i].wait_recv()
            both = partial_ref[owner * owned + i] + near_ref[at]
            if d == 0:
                out_ref[i] = both
                continue
            sum_ref[at - owned] = both
            far[d, i] = pltpu.make_async_remote_copy(
                src_ref=sum_ref.at[at - owned],
                dst_ref=far_ref.at[at - owned],
                send_sem=far_send.at[at - owned],
                recv_sem=far_recv.at[at - owned],
                device_id={"toa": owner},
                device_id_type=MESH,
            )
            far[d, i].start()
    pad_ref[...] = jnp.zeros_like(pad_ref)
    pad_ref[0 : directions_ref.shape[0], :] = directions_ref[...]
    coupling_ref[...] = coupling_inverse(pad_ref[...], owned)
    for (d, i), copy in far.items():
        copy.wait_recv()
        out_ref[i] += far_ref[d * owned + i - owned]
    for copy in list(near.values()) + list(far.values()):
        copy.wait_send()


def reduce_owners(partial, directions, toa_devices):
    pulsars, height, lanes = partial.shape
    number = directions.shape[1]
    owned = pulsars // toa_devices
    chips = toa_devices // 2
    moved = owned * (chips - 1)
    block = (height, lanes)
    vmem = pl.BlockSpec(memory_space=pltpu.VMEM)
    return pl.pallas_call(
        functools.partial(reduce_kernel, chips),
        out_shape=(
            jax.ShapeDtypeStruct((owned,) + block, jnp.float32),
            jax.ShapeDtypeStruct((number, LANES), jnp.float32),
        ),
        in_specs=[vmem, vmem],
        out_specs=(vmem, vmem),
        scratch_shapes=[
            pltpu.VMEM((owned * chips,) + block, jnp.float32),
            pltpu.VMEM((moved,) + block, jnp.float32),
            pltpu.VMEM((moved,) + block, jnp.float32),
            pltpu.VMEM((8, number), jnp.float32),
            pltpu.SemaphoreType.DMA((owned * chips,)),
            pltpu.SemaphoreType.DMA((owned * chips,)),
            pltpu.SemaphoreType.DMA((moved,)),
            pltpu.SemaphoreType.DMA((moved,)),
        ],
        compiler_params=pltpu.CompilerParams(collective_id=0, has_side_effects=True),
        cost_estimate=pl.CostEstimate(flops=4 * pulsars * height * lanes, bytes_accessed=40 * pulsars * height * lanes, transcendentals=0),
        name="reduce_owners",
    )(partial, directions)


def paired(block):
    side, lanes = block.shape
    left = iota((side, lanes), 1) < side
    return jnp.concatenate([jnp.where(left, block, 0.0), jnp.where(left, 0.0, block)], axis=0)


def dot_paired(a, block):
    return dot(a, paired(block))


def dot_paired_t(a, block):
    return lax.dot_general(
        a, paired(block), (((1,), (1,)), ((), ())), precision=highest, preferred_element_type=jnp.float32
    )


def halves(row, side):
    left = iota(row.shape, 1) < side
    return [
        jnp.sum(jnp.where(left, row, 0.0), axis=1, keepdims=True),
        jnp.sum(jnp.where(left, 0.0, row), axis=1, keepdims=True),
    ]


def payload_rows(owned):
    return -(-17 * owned // 8) * 8


def eliminate(devices, device, sums_ref, prior_ref, coupling_ref, spectrum_ref, packed_ref, facts_ref):
    owned, height, lanes = sums_ref.shape
    side = SIDE
    columns = height - 8
    blocks = columns // side
    lane = iota((1, lanes), 1)
    left = lane < side
    row2 = iota((side, lanes), 0)
    col2 = lax.rem(iota((side, lanes), 1), side)
    freqs = spectrum_ref.shape[1]
    pick = jnp.where(iota((freqs, lanes), 0) == lax.rem(iota((freqs, lanes), 1), side) // 2, 1.0, 0.0)
    power2 = dot(jnp.broadcast_to(1.0 / spectrum_ref[...], (8, freqs)), pick)[0:1]
    row1, col1 = iota((lanes, lanes), 0), iota((lanes, lanes), 1)
    packed_ref[...] = jnp.zeros_like(packed_ref)
    for first in range(0, owned, 2):
        pair = (first, min(first + 1, owned - 1))
        whole = []
        for p in pair:
            mixed = sums_ref[p, 0:lanes, :]
            turned = jnp.transpose(mixed)
            diag = sums_ref[p, columns + 4 : columns + 5, :]
            top = jnp.where(row1 >= col1, mixed, turned)
            low = jnp.where(row1 < col1, mixed, jnp.where(row1 == col1, diag, turned))
            whole.append({(0, 0): top, (0, 1): sums_ref[p, lanes : 2 * lanes, :], (1, 1): low})

        def join(parts, j):
            if j % 2 == 0:
                return jnp.where(left, parts[0], pltpu.roll(parts[1], side, 1))
            return jnp.where(left, pltpu.roll(parts[0], side, 1), parts[1])

        def both(i, j):
            lo = (i % 2) * side
            return join([w[i // 2, j // 2][lo : lo + side] for w in whole], j)

        order = list(range(blocks - 1, -1, -1))
        a = {}
        for s, j in enumerate(order):
            for i in order[s:]:
                a[i, j] = both(i, j)
            at = columns + j // 2
            a["p", j] = join([jnp.broadcast_to(sums_ref[p, at : at + 1, :], (8, lanes)) for p in pair], j)
            if j:
                own = jnp.concatenate([1.0 / prior_ref[p : p + 1, (j - 1) * side : j * side] for p in pair], axis=1)
                a[j, j] = a[j, j] + jnp.where(row2 == col2, own, 0.0)
        logs = jnp.zeros((1, lanes), jnp.float32)
        quads = jnp.zeros((1, lanes), jnp.float32)
        for s, j in enumerate(order[:-1]):
            inverse, extra_logs = invert_pair(a[j, j], PANEL)
            logs = logs + extra_logs
            rest = order[s + 1 :]
            scaled = {i: dot_paired(a[i, j], inverse) for i in rest + ["p"]}
            quads = quads + scaled["p"][0:1] * a["p", j][0:1]
            for t, m in enumerate(rest):
                for i in rest[t:] + ["p"]:
                    a[i, m] = a[i, m] - dot_paired_t(scaled[i], a[m, j])
        owns = []
        for h, p in enumerate(pair):
            at = (p * devices) + device
            line = coupling_ref[pl.ds(at, 1), :]
            here = lane == at
            owns.append(jnp.sum(jnp.where(here, line, 0.0), axis=1, keepdims=True))
        own2 = jnp.where(left, owns[0], owns[1])
        x, extra_logs = invert_pair(a[0, 0] + jnp.where(row2 == col2, own2 * power2, 0.0), PANEL)
        logs = halves(logs + extra_logs, side)
        quads = halves(quads, side)
        row3, col3 = row2[:HALF], col2[:HALF]
        bottom = pltpu.roll(x[HALF:], lanes - HALF, 1)
        packed = jnp.where((col3 < HALF) & (row3 < col3), bottom, x[:HALF])
        diag = jnp.sum(jnp.where(row3 + HALF == col3, x[HALF:], 0.0), axis=0, keepdims=True)
        target = a["p", 0][0:1]
        turned = pltpu.roll(packed, side, 1)
        quarter = HALF // 2
        for h, p in enumerate(pair[: min(2, owned - first)]):
            tail = sums_ref[p, columns + 2 : columns + 4, :]
            energy = jnp.sum(tail[0:1], axis=1, keepdims=True)
            count = jnp.sum(tail[1:2], axis=1, keepdims=True)
            if h == 0:
                mine = jnp.where(left, packed[:quarter], turned[quarter:])
                line = jnp.where(left, target, pltpu.roll(diag, HALF, 1))
            else:
                mine = jnp.where(left, turned[:quarter], packed[quarter:])
                line = jnp.where(left, pltpu.roll(target, side, 1), pltpu.roll(diag, lanes - HALF, 1))
            packed_ref[p * quarter : (p + 1) * quarter, :] = mine
            at = owned * quarter + p
            packed_ref[at : at + 1, :] = line
            facts = jnp.where(lane == side, logs[h] / columns, line)
            facts = jnp.where(lane == side + 1, energy - quads[h], facts)
            facts = jnp.where(lane == side + 2, count, facts)
            facts_ref[p : p + 1, :] = facts


def total(x):
    return jnp.sum(jnp.sum(x, axis=0, keepdims=True), axis=1, keepdims=True)


def split(x):
    high = x.astype(jnp.bfloat16)
    return high, (x - high.astype(jnp.float32)).astype(jnp.bfloat16)


def conjugate(all_ref, coupling_ref, spectrum_ref, turned_ref, blocks_ref, w_ref, devices, owned):
    number = devices * owned
    rows = payload_rows(owned)
    quarter = HALF // 2
    fold = LANES // number

    def across(at):
        parts = [all_ref[pl.ds(begin, devices, stride=rows), :] for begin in at]
        return jnp.transpose(jnp.concatenate(parts * fold, axis=0))

    def turn(r, carry):
        x = across([h * quarter + r for h in range(owned)])
        turned_ref[pl.ds(pl.multiple_of(r * SIDE, SIDE), SIDE), :] = x[:SIDE]
        turned_ref[pl.ds(pl.multiple_of((r + quarter) * SIDE, SIDE), SIDE), :] = x[SIDE:]
        return carry

    for r in range(quarter):
        turn(r, 0)
    x = across([owned * quarter + h for h in range(owned)])
    target, diag = x[:SIDE], x[SIDE : SIDE + HALF]
    left = iota((HALF, LANES), 1) < SIDE
    sub = iota((HALF, LANES), 0)

    for r in range(HALF):
        mine = turned_ref[r * SIDE : r * SIDE + HALF, :]
        beside = turned_ref[r * SIDE + HALF : (r + 1) * SIDE, :]
        mirror = turned_ref[pl.ds(r, HALF, stride=SIDE), :]
        below = turned_ref[pl.ds(r + HALF, HALF, stride=SIDE), :]
        first = jnp.where(sub <= r, mine, mirror)
        last = jnp.where(sub > r, mine, jnp.where(sub == r, diag, mirror))
        if fold == 2:
            blocks_ref[r, 0:HALF, :] = jnp.where(left, first, below)
            blocks_ref[r, HALF:SIDE, :] = jnp.where(left, beside, last)
        else:
            blocks_ref[r, 0:HALF, :] = first
            blocks_ref[r, HALF:SIDE, :] = beside
            blocks_ref[r + HALF, 0:HALF, :] = below
            blocks_ref[r + HALF, HALF:SIDE, :] = last

    coupling = coupling_ref[...]
    row, col = iota(coupling.shape, 0), iota(coupling.shape, 1)
    high, low = split(jnp.where(row == lax.rem(col, number), 0.0, coupling))
    freqs = spectrum_ref.shape[1]
    place = jnp.where(iota((SIDE, freqs), 0) // 2 == iota((SIDE, freqs), 1), 1.0 / spectrum_ref[...], 0.0)
    power = dot(place, jnp.ones((freqs, LANES), jnp.float32))
    wide = iota((SIDE, LANES), 1) < SIDE

    def mix(v):
        top, rest = split(v)
        if fold == 2:
            x = jnp.where(wide, top.astype(jnp.float32), rest.astype(jnp.float32)).astype(jnp.bfloat16)
            out = jnp.dot(
                jnp.concatenate([x, x], axis=1),
                jnp.concatenate([high, high, low, low], axis=0),
                preferred_element_type=jnp.float32,
            )
        else:
            x = jnp.concatenate([top, rest], axis=1)
            out = jnp.dot(x, jnp.concatenate([high, high], axis=0), preferred_element_type=jnp.float32)
            out = out + jnp.dot(x, jnp.concatenate([low, low], axis=0), preferred_element_type=jnp.float32)
        return power * out

    def apply_blocks(v):
        if fold == 2:
            w_ref[0:HALF, :] = jnp.where(left, v[:HALF], v[HALF:])
        else:
            w_ref[...] = v
        acc = jnp.zeros((SIDE, LANES), jnp.float32)
        for k in range(SIDE // fold):
            acc = acc + blocks_ref[k] * w_ref[k : k + 1, :]
        return acc + pltpu.roll(acc, SIDE, 1) if fold == 2 else acc

    residual = target
    scaled = apply_blocks(residual)
    inner = total(residual * scaled)
    mixed = mix(scaled)
    solved = apply_blocks(mixed)
    direction, block_direction = scaled, residual
    solution = jnp.zeros((SIDE, LANES), jnp.float32)
    for iteration in range(ITERS):
        mapped = block_direction + mixed
        step = inner / total(direction * mapped)
        solution = solution + step * direction
        if iteration + 1 == ITERS:
            break
        residual = residual - step * mapped
        scaled = scaled - step * (direction + solved)
        following = total(residual * scaled)
        ratio = following / inner
        fresh = mix(scaled)
        if iteration + 2 < ITERS:
            solved = apply_blocks(fresh) + ratio * solved
        mixed = fresh + ratio * mixed
        direction = scaled + ratio * direction
        block_direction = residual + ratio * block_direction
        inner = following
    return solution


def gather_kernel(
    groups, chips, sums_ref, prior_ref, coupling_ref, spectrum_ref, out_ref,
    mine_ref, facts_ref, all_ref, turned_ref, blocks_ref, w_ref, final_ref, psr_send, chip_send, core_send, recv
):
    psr, me = lax.axis_index("psr"), lax.axis_index("toa")
    toa_devices = 2 * chips
    devices = groups * toa_devices
    core = lax.rem(me, 2)
    chip = me // 2
    other = 1 - core
    partner = chip * 2 + other
    rows = mine_ref.shape[0]
    owned = out_ref.shape[0]
    barrier = pltpu.get_barrier_semaphore()

    def greet(psr_to, toa_to):
        pl.semaphore_signal(barrier, inc=1, device_id={"psr": psr_to, "toa": toa_to}, device_id_type=MESH)

    greet(psr, partner)
    for d in range(1, chips):
        greet(psr, lax.rem(chip + d, chips) * 2 + core)
    for e in range(1, groups):
        greet(lax.rem(psr + e, groups), me)
    own = psr * toa_devices + me
    eliminate(devices, own, sums_ref, prior_ref, coupling_ref, spectrum_ref, mine_ref, facts_ref)
    pl.semaphore_wait(barrier, chips + groups - 1)
    sent = []

    def block_of(e, toa):
        return lax.rem(psr + groups - e, groups) * toa_devices + toa

    def slot(block):
        return all_ref.at[pl.ds(pl.multiple_of(block * rows, 8), rows)]

    def copy(source, block, sem, psr_to, toa_to):
        return pltpu.make_async_remote_copy(
            src_ref=source,
            dst_ref=slot(block),
            send_sem=sem,
            recv_sem=recv.at[block],
            device_id={"psr": psr_to, "toa": toa_to},
            device_id_type=MESH,
        )

    def send(source, block, sem, psr_to, toa_to):
        moving = copy(source, block, sem, psr_to, toa_to)
        moving.start()
        sent.append(moving)

    def arrived(block):
        copy(slot(block), block, core_send.at[0], psr, partner).wait_recv()

    for e in range(1, groups):
        send(mine_ref, own, psr_send.at[e - 1], lax.rem(psr + e, groups), me)
    for e in range(groups):
        block = block_of(e, me)
        if e:
            arrived(block)
        source = slot(block) if e else mine_ref
        for d in range(1, chips):
            send(source, block, chip_send.at[e * (chips - 1) + d - 1], psr, lax.rem(chip + d, chips) * 2 + core)
        send(source, block, core_send.at[e], psr, partner)
    for d in range(1, chips):
        for e in range(groups):
            block = block_of(e, lax.rem(chip + chips - d, chips) * 2 + core)
            arrived(block)
            send(slot(block), block, core_send.at[d * groups + e], psr, partner)
    all_ref[pl.ds(pl.multiple_of(own * rows, 8), rows), :] = mine_ref[...]
    for c in range(chips):
        for e in range(groups):
            arrived(block_of(e, c * 2 + other))
    for moving in sent:
        moving.wait_send()
    solution = conjugate(all_ref, coupling_ref, spectrum_ref, turned_ref, blocks_ref, w_ref, devices, owned)
    final_ref[...] = jnp.transpose(jnp.concatenate([solution, solution], axis=0))
    lane = iota((1, LANES), 1)
    for h in range(owned):
        mine = final_ref[pl.ds(h * devices + own, 1), :]
        facts = facts_ref[h : h + 1, :]
        fit = jnp.sum(jnp.where(lane < SIDE, facts * mine, 0.0), axis=1, keepdims=True)

        def at(k):
            return jnp.sum(jnp.where(lane == SIDE + k, facts, 0.0), axis=1, keepdims=True)

        chi_square = (at(1) - fit) / at(2)
        line = jnp.where(lane < SIDE, mine, jnp.where(lane == SIDE, at(0), chi_square))
        out_ref[h : h + 1, :] = line


def finish(sums, own_prior, coupling, spectrum, groups, toa_devices):
    chips = toa_devices // 2
    devices = groups * toa_devices
    owned = sums.shape[0]
    rows = payload_rows(owned)
    fold = LANES // (devices * owned)
    vmem = pl.BlockSpec(memory_space=pltpu.VMEM)
    return pl.pallas_call(
        functools.partial(gather_kernel, groups, chips),
        out_shape=jax.ShapeDtypeStruct((owned, LANES), jnp.float32),
        in_specs=[vmem] * 4,
        out_specs=vmem,
        scratch_shapes=[
            pltpu.VMEM((rows, LANES), jnp.float32),
            pltpu.VMEM((owned, LANES), jnp.float32),
            pltpu.VMEM((devices * rows, LANES), jnp.float32),
            pltpu.VMEM((HALF * SIDE, LANES), jnp.float32),
            pltpu.VMEM((SIDE // fold, SIDE, LANES), jnp.float32),
            pltpu.VMEM((SIDE, LANES), jnp.float32),
            pltpu.VMEM((LANES, LANES), jnp.float32),
            pltpu.SemaphoreType.DMA((groups - 1,)),
            pltpu.SemaphoreType.DMA((groups * (chips - 1),)),
            pltpu.SemaphoreType.DMA((groups * chips,)),
            pltpu.SemaphoreType.DMA((devices,)),
        ],
        compiler_params=pltpu.CompilerParams(collective_id=1, has_side_effects=True),
        name="finish",
    )(sums, own_prior, coupling, spectrum)


def body(design, noise_weight, residuals, slot_pulsar, slot_rows, own_prior, spectrum, directions):
    groups, toa_devices = lax.axis_size("psr"), lax.axis_size("toa")
    partial = local_grams(design, noise_weight, residuals, slot_pulsar, slot_rows)
    sums, coupling = reduce_owners(partial, directions, toa_devices)
    lines = finish(sums, own_prior, coupling, spectrum[None, :], groups, toa_devices)
    return (lines[:, :SIDE], lines[:, SIDE], lines[:, SIDE + 1])


def solution(mesh):
    return jax.shard_map(
        body,
        mesh=mesh,
        in_specs=(
            P(("psr", "toa"), None, None),
            P(("psr", "toa"), None),
            P(("psr", "toa"), None),
            P(("psr", "toa")),
            P(("psr", "toa")),
            P(("psr", "toa"), None),
            P(),
            P(),
        ),
        out_specs=(P(("psr", "toa"), None), P(("psr", "toa")), P(("psr", "toa"))),
        check_vma=False,
    )
```

```python
import functools

import jax
import jax.numpy as jnp
from jax import lax
from jax.experimental import pallas as pl
from jax.experimental.pallas import tpu as pltpu
from jax.sharding import PartitionSpec as P

GROUP_PULSARS = 8
ITERS = 8
SIDE = 64
HALF = 32
LANES = 128
STEP_SLOTS = 32
CHUNK_SLOTS = 8
PANEL = 16
highest = lax.Precision.HIGHEST
MESH = pl.DeviceIdType.MESH


def dot(a, b, precision=highest):
    return jnp.dot(a, b, precision=precision, preferred_element_type=jnp.float32)


def iota(shape, axis):
    return lax.broadcasted_iota(jnp.int32, shape, axis)


def gram_kernel(pulsar_ref, rows_ref, design_ref, weight_ref, residual_ref, out_ref, acc_ref, acc2_ref, held_ref, sems):
    slots, toas, columns = design_ref.shape
    half = columns // 2
    chunks = slots // CHUNK_SLOTS

    def chunk(c):
        at = pl.ds(pl.multiple_of(c * CHUNK_SLOTS, CHUNK_SLOTS), CHUNK_SLOTS)
        return pltpu.make_async_copy(design_ref.at[at], held_ref.at[at], sems.at[c])

    for c in range(chunks):
        chunk(c).start()
    acc_ref[...] = jnp.zeros_like(acc_ref)
    acc2_ref[...] = jnp.zeros_like(acc2_ref)
    lanes = iota((1, toas), 1)
    at_row = iota((8, half), 0)

    def step(s, carry):
        for c in range(STEP_SLOTS // CHUNK_SLOTS):
            chunk(s * (STEP_SLOTS // CHUNK_SLOTS) + c).wait()
        base = pl.multiple_of(s * STEP_SLOTS, STEP_SLOTS)
        weights = weight_ref[pl.ds(base, STEP_SLOTS), :]
        residuals = residual_ref[pl.ds(base, STEP_SLOTS), :].astype(jnp.float32)
        for j in range(STEP_SLOTS):
            slot = base + j
            p = pulsar_ref[slot]
            into = acc_ref if j % 2 == 0 else acc2_ref
            valid = lanes < rows_ref[slot]
            weight = jnp.where(valid, weights[j : j + 1, :], 0.0)
            residual = residuals[j : j + 1, :]
            block = held_ref[slot]
            across = jnp.transpose(block).astype(jnp.float32)
            weighted = (across * weight).astype(jnp.bfloat16)
            gram = jnp.dot(weighted, block, preferred_element_type=jnp.float32)
            spread = jnp.broadcast_to(residual, (8, toas)).astype(jnp.bfloat16)
            fitted = lax.dot_general(
                spread, weighted, (((1,), (1,)), ((), ())), preferred_element_type=jnp.float32
            )
            energy = weight * residual * residual
            count = jnp.where(valid, 1.0, 0.0)
            extra = jnp.where(at_row == 0, fitted[:, :half], jnp.where(at_row == 1, fitted[:, half:], 0.0))
            extra = jnp.where(at_row == 2, energy, jnp.where(at_row == 3, count, extra))
            into[p, 0:half, :] += gram[:half, :half]
            into[p, half:columns, :] += gram[:half, half:]
            into[p, columns : columns + half, :] += gram[half:, half:]
            into[p, columns + half : columns + half + 8, :] += extra
        return carry

    lax.fori_loop(0, slots // STEP_SLOTS, step, 0)
    row, col = iota((half, half), 0), iota((half, half), 1)

    def both(p, lo, hi):
        return acc_ref[p, lo:hi, :] + acc2_ref[p, lo:hi, :]

    def pack(p, carry):
        low = both(p, columns, columns + half)
        out_ref[p, 0:half, :] = jnp.where(row >= col, both(p, 0, half), low)
        out_ref[p, half + 8 : columns + 8, :] = both(p, half, columns)
        diag = jnp.sum(jnp.where(row == col, low, 0.0), axis=0, keepdims=True)
        tail = both(p, columns + half, columns + half + 8)
        out_ref[p, half : half + 8, :] = jnp.where(at_row == 4, diag, tail)
        return carry

    lax.fori_loop(0, GROUP_PULSARS, pack, 0)


def local_grams(design, noise_weight, residuals, slot_pulsar, slot_rows):
    slots, toas, columns = design.shape
    half = columns // 2
    smem = pl.BlockSpec(memory_space=pltpu.SMEM)
    vmem = pl.BlockSpec(memory_space=pltpu.VMEM)
    return pl.pallas_call(
        gram_kernel,
        in_specs=[smem, smem, pl.BlockSpec(memory_space=pltpu.HBM), vmem, vmem],
        out_specs=vmem,
        out_shape=pltpu.VMEM((GROUP_PULSARS, columns + 8, half), jnp.float32),
        scratch_shapes=[
            pltpu.VMEM((GROUP_PULSARS, columns + half + 8, half), jnp.float32),
            pltpu.VMEM((GROUP_PULSARS, columns + half + 8, half), jnp.float32),
            pltpu.VMEM((slots, toas, columns), jnp.bfloat16),
            pltpu.SemaphoreType.DMA((slots // CHUNK_SLOTS,)),
        ],
        compiler_params=pltpu.CompilerParams(vmem_limit_bytes=54 * 2**20),
        name="gram",
    )(slot_pulsar, slot_rows, design, noise_weight, residuals)


def invert_pair(x, width):
    side, lanes = x.shape
    within = lax.rem(iota((1, lanes), 1), side)
    half = iota((side, lanes), 1)
    half = half - lax.rem(half, side)
    sub = iota((width, lanes), 0)
    pivots = jnp.ones((1, lanes), jnp.float32)
    for lo in range(0, side, width):
        hi = lo + width
        columns = [jnp.take_along_axis(x, half + (lo + k), axis=1) for k in range(width)]
        rows = x[lo:hi]
        inner = [c[lo:hi] for c in columns]
        for k in range(width):
            here = within == lo + k
            pivot = inner[k][k : k + 1]
            inverse = 1.0 / pivot
            pivots = jnp.where(here, pivot, pivots)
            row = jnp.where(here, 1.0, rows[k : k + 1]) * inverse
            at = sub == k
            rows = jnp.where(at, row, jnp.where(here, 0.0, rows) - inner[k] * row)
            for j in range(k + 1, width):
                scaled = inner[j][k : k + 1] * inverse
                inner[j] = jnp.where(at, scaled, inner[j] - inner[k] * scaled)
        inside = (within >= lo) & (within < hi)
        parts = []
        for begin in range(0, side, width):
            if begin == lo:
                parts.append(rows)
                continue
            acc = jnp.where(inside, 0.0, x[begin : begin + width])
            for k in range(width):
                acc = acc - columns[k][begin : begin + width] * rows[k : k + 1]
            parts.append(acc)
        x = jnp.concatenate(parts, axis=0)
    return x, jnp.log(pivots)


def coupling_inverse(directions, owned):
    number = directions.shape[1]
    row, col = iota((number, number), 0), iota((number, number), 1)
    if owned > 1:
        devices = number // owned
        source = lax.rem(col, devices) * owned + col // devices
        directions = dot(directions, jnp.where(row == source, 1.0, 0.0))
    cosines = lax.dot_general(
        directions, directions, (((0,), (0,)), ((), ())), precision=highest, preferred_element_type=jnp.float32
    )
    cosines = jnp.clip(cosines, -1.0, 1.0)
    spread = jnp.where(row == col, 1.0, 0.5 * (1.0 - cosines))
    curve = 1.5 * spread * jnp.log(spread) - 0.25 * spread + 0.5
    x = jnp.where(row == col, 1.0, curve)
    if number == SIDE:
        return invert_pair(jnp.concatenate([x, x], axis=1), PANEL)[0]
    tiles = number // SIDE
    for b in range(tiles):
        lo, hi = b * SIDE, (b + 1) * SIDE
        block = x[lo:hi, lo:hi]
        inverse = invert_pair(jnp.concatenate([block, block], axis=1), PANEL)[0][:, :SIDE]
        across = dot(inverse, x[lo:hi, :])
        down = x[:, lo:hi]
        inside_row = (row >= lo) & (row < hi)
        inside_col = (col >= lo) & (col < hi)
        updated = x - dot(down, across)
        placed = -dot(down, inverse)
        updated = jnp.where(inside_col, jnp.concatenate([placed] * tiles, axis=1), updated)
        fixed = jnp.where(
            inside_col,
            jnp.concatenate([jnp.concatenate([inverse] * tiles, axis=1)] * tiles, axis=0),
            jnp.concatenate([across] * tiles, axis=0),
        )
        x = jnp.where(inside_row, fixed, updated)
    return x


def paired(block):
    side, lanes = block.shape
    left = iota((side, lanes), 1) < side
    return jnp.concatenate([jnp.where(left, block, 0.0), jnp.where(left, 0.0, block)], axis=0)


def dot_paired(a, block):
    return dot(a, paired(block))


def dot_paired_t(a, block):
    return lax.dot_general(
        a, paired(block), (((1,), (1,)), ((), ())), precision=highest, preferred_element_type=jnp.float32
    )


def halves(row, side):
    left = iota(row.shape, 1) < side
    return [
        jnp.sum(jnp.where(left, row, 0.0), axis=1, keepdims=True),
        jnp.sum(jnp.where(left, 0.0, row), axis=1, keepdims=True),
    ]


def unpack(mixed, diag, upper):
    row, col = iota(mixed.shape, 0), iota(mixed.shape, 1)
    turned = jnp.transpose(mixed)
    if upper:
        return jnp.where(row >= col, mixed, turned)
    return jnp.where(row < col, mixed, jnp.where(row == col, diag, turned))


def join(parts, j, side):
    left = iota(parts[0].shape, 1) < side
    if j % 2 == 0:
        return jnp.where(left, parts[0], pltpu.roll(parts[1], side, 1))
    return jnp.where(left, pltpu.roll(parts[0], side, 1), parts[1])


def with_prior(block, prior_ref, pair, j):
    side, lanes = block.shape
    row, col = iota((side, lanes), 0), lax.rem(iota((side, lanes), 1), side)
    own = jnp.concatenate([1.0 / prior_ref[p : p + 1, (j - 1) * side : j * side] for p in pair], axis=1)
    return block + jnp.where(row == col, own, 0.0)


def pair_of(first, owned):
    return (first, min(first + 1, owned - 1))


def reduce_kernel(
    chips, partial_ref, directions_ref, prior_ref, out_ref, coupling_ref, early_ref, near_ref, sum_ref, far_ref, pad_ref,
    near_send, near_recv, far_send, far_recv
):
    me = lax.axis_index("toa")
    core = lax.rem(me, 2)
    chip = me // 2
    other = 1 - core
    owned, height, lanes = out_ref.shape
    side = SIDE
    pieces = ((side, lanes + 8), (0, side), (lanes + 8, height))
    barrier = pltpu.get_barrier_semaphore()
    pl.semaphore_signal(barrier, inc=1, device_id={"toa": chip * 2 + other}, device_id_type=MESH)
    for d in range(1, chips):
        target = lax.rem(chip + d, chips) * 2 + core
        pl.semaphore_signal(barrier, inc=1, device_id={"toa": target}, device_id_type=MESH)
    pl.semaphore_wait(barrier, chips)
    order = [(d % chips, i, q) for d in range(1, chips) for q in range(3) for i in range(owned)]
    order += [(0, i, q) for q in range(3) for i in range(owned)]
    near, far = {}, {}
    for d, i, q in order:
        owner = lax.rem(chip + d, chips) * 2 + other
        at, (lo, hi) = d * owned + i, pieces[q]
        near[d, i, q] = pltpu.make_async_remote_copy(
            src_ref=partial_ref.at[owner * owned + i, lo:hi],
            dst_ref=near_ref.at[at, lo:hi],
            send_sem=near_send.at[at, q],
            recv_sem=near_recv.at[at, q],
            device_id={"toa": chip * 2 + other},
            device_id_type=MESH,
        )
        near[d, i, q].start()
    for d, i, q in order:
        owner = lax.rem(chip + d, chips) * 2 + core
        at, (lo, hi) = d * owned + i, pieces[q]
        near[d, i, q].wait_recv()
        both = partial_ref[owner * owned + i, lo:hi] + near_ref[at, lo:hi]
        if d == 0:
            out_ref[i, lo:hi] = both
            continue
        sum_ref[at - owned, lo:hi] = both
        far[d, i, q] = pltpu.make_async_remote_copy(
            src_ref=sum_ref.at[at - owned, lo:hi],
            dst_ref=far_ref.at[at - owned, lo:hi],
            send_sem=far_send.at[at - owned, q],
            recv_sem=far_recv.at[at - owned, q],
            device_id={"toa": owner},
            device_id_type=MESH,
        )
        far[d, i, q].start()
    pad_ref[...] = jnp.zeros_like(pad_ref)
    pad_ref[0 : directions_ref.shape[0], :] = directions_ref[...]
    coupling_ref[...] = coupling_inverse(pad_ref[...], owned)

    def collect(q):
        lo, hi = pieces[q]
        for d, i, which in order:
            if d and which == q:
                far[d, i, q].wait_recv()
                out_ref[i, lo:hi] += far_ref[(d - 1) * owned + i, lo:hi]

    pairs = [pair_of(first, owned) for first in range(0, owned, 2)]
    corner = lax.broadcasted_iota(jnp.int32, (side, lanes), 0) - iota((side, lanes), 1) + side
    collect(0)
    firsts = []
    for n, pair in enumerate(pairs):
        parts = []
        for p in pair:
            mixed, diag = out_ref[p, side:lanes], out_ref[p, lanes + 4 : lanes + 5]
            turned = jnp.transpose(jnp.concatenate([mixed, mixed], axis=0))[side:]
            turned = jnp.concatenate([turned[:, :side], turned[:, :side]], axis=1)
            parts.append(jnp.where(corner < 0, mixed, jnp.where(corner == 0, diag, turned)))
        inverse, logs = invert_pair(with_prior(join(parts, 1, side), prior_ref, pair, 3), PANEL)
        early_ref[n, 0:side, :] = inverse
        firsts.append((inverse, logs))
    collect(1)
    for n, pair in enumerate(pairs):
        low = [unpack(out_ref[p, 0:lanes], out_ref[p, lanes + 4 : lanes + 5], False) for p in pair]
        inverse, logs = firsts[n]
        cross = join([x[:side] for x in low], 1, side)
        before = with_prior(join([x[:side] for x in low], 0, side), prior_ref, pair, 2)
        scaled = dot_paired(cross, inverse)
        inverse, more = invert_pair(before - dot_paired_t(scaled, cross), PANEL)
        early_ref[n, side : 2 * side, :] = inverse
        early_ref[n, 2 * side :, :] = jnp.broadcast_to(logs + more, (8, lanes))
    collect(2)
    for copy in list(near.values()) + list(far.values()):
        copy.wait_send()


def reduce_owners(partial, directions, own_prior, toa_devices):
    pulsars, height, lanes = partial.shape
    number = directions.shape[1]
    owned = pulsars // toa_devices
    chips = toa_devices // 2
    moved = owned * (chips - 1)
    block = (height, lanes)
    vmem = pl.BlockSpec(memory_space=pltpu.VMEM)
    return pl.pallas_call(
        functools.partial(reduce_kernel, chips),
        out_shape=(
            jax.ShapeDtypeStruct((owned,) + block, jnp.float32),
            jax.ShapeDtypeStruct((number, LANES), jnp.float32),
            jax.ShapeDtypeStruct(((owned + 1) // 2, 2 * SIDE + 8, LANES), jnp.float32),
        ),
        in_specs=[vmem] * 3,
        out_specs=(vmem,) * 3,
        scratch_shapes=[
            pltpu.VMEM((owned * chips,) + block, jnp.float32),
            pltpu.VMEM((moved,) + block, jnp.float32),
            pltpu.VMEM((moved,) + block, jnp.float32),
            pltpu.VMEM((8, number), jnp.float32),
            pltpu.SemaphoreType.DMA((owned * chips, 3)),
            pltpu.SemaphoreType.DMA((owned * chips, 3)),
            pltpu.SemaphoreType.DMA((moved, 3)),
            pltpu.SemaphoreType.DMA((moved, 3)),
        ],
        compiler_params=pltpu.CompilerParams(collective_id=0, has_side_effects=True, vmem_limit_bytes=20 * 2**20),
        cost_estimate=pl.CostEstimate(flops=4 * pulsars * height * lanes, bytes_accessed=40 * pulsars * height * lanes, transcendentals=0),
        name="reduce_owners",
    )(partial, directions, own_prior)


def payload_rows(owned):
    return -(-17 * owned // 8) * 8


def eliminate(devices, device, sums_ref, early_ref, prior_ref, coupling_ref, spectrum_ref, packed_ref, facts_ref):
    owned, height, lanes = sums_ref.shape
    side = SIDE
    columns = height - 8
    blocks = columns // side
    lane = iota((1, lanes), 1)
    left = lane < side
    row2 = iota((side, lanes), 0)
    col2 = lax.rem(iota((side, lanes), 1), side)
    freqs = spectrum_ref.shape[1]
    pick = jnp.where(iota((freqs, lanes), 0) == lax.rem(iota((freqs, lanes), 1), side) // 2, 1.0, 0.0)
    power2 = dot(jnp.broadcast_to(1.0 / spectrum_ref[...], (8, freqs)), pick)[0:1]
    packed_ref[...] = jnp.zeros_like(packed_ref)
    for first in range(0, owned, 2):
        pair = pair_of(first, owned)
        whole = []
        for p in pair:
            mixed, diag = sums_ref[p, 0:lanes, :], sums_ref[p, lanes + 4 : lanes + 5, :]
            whole.append({
                (0, 0): unpack(mixed, diag, True),
                (0, 1): sums_ref[p, lanes + 8 : 2 * lanes + 8, :],
                (1, 1): unpack(mixed, diag, False),
            })

        def both(i, j):
            lo = (i % 2) * side
            return join([w[i // 2, j // 2][lo : lo + side] for w in whole], j, side)

        order = list(range(blocks - 1, -1, -1))
        a = {}
        for s, j in enumerate(order):
            for i in order[s:]:
                a[i, j] = both(i, j)
            at = lanes + j // 2
            a["p", j] = join([jnp.broadcast_to(sums_ref[p, at : at + 1, :], (8, lanes)) for p in pair], j, side)
        a[1, 1] = with_prior(a[1, 1], prior_ref, pair, 1)
        early = early_ref.at[first // 2]
        logs = early[2 * side : 2 * side + 1, :]
        quads = jnp.zeros((1, lanes), jnp.float32)
        for s, j in enumerate(order[:-1]):
            if s < 2:
                inverse = early[s * side : (s + 1) * side, :]
            else:
                inverse, extra_logs = invert_pair(a[j, j], PANEL)
                logs = logs + extra_logs
            rest = order[s + 1 :]
            scaled = {i: dot_paired(a[i, j], inverse) for i in rest + ["p"]}
            quads = quads + scaled["p"][0:1] * a["p", j][0:1]
            for t, m in enumerate(rest):
                for i in rest[t:] + ["p"]:
                    a[i, m] = a[i, m] - dot_paired_t(scaled[i], a[m, j])
        owns = []
        for h, p in enumerate(pair):
            at = (p * devices) + device
            line = coupling_ref[pl.ds(at, 1), :]
            here = lane == at
            owns.append(jnp.sum(jnp.where(here, line, 0.0), axis=1, keepdims=True))
        own2 = jnp.where(left, owns[0], owns[1])
        x, extra_logs = invert_pair(a[0, 0] + jnp.where(row2 == col2, own2 * power2, 0.0), PANEL)
        logs = halves(logs + extra_logs, side)
        quads = halves(quads, side)
        row3, col3 = row2[:HALF], col2[:HALF]
        bottom = pltpu.roll(x[HALF:], lanes - HALF, 1)
        packed = jnp.where((col3 < HALF) & (row3 < col3), bottom, x[:HALF])
        diag = jnp.sum(jnp.where(row3 + HALF == col3, x[HALF:], 0.0), axis=0, keepdims=True)
        target = a["p", 0][0:1]
        turned = pltpu.roll(packed, side, 1)
        quarter = HALF // 2
        for h, p in enumerate(pair[: min(2, owned - first)]):
            tail = sums_ref[p, lanes + 2 : lanes + 4, :]
            energy = jnp.sum(tail[0:1], axis=1, keepdims=True)
            count = jnp.sum(tail[1:2], axis=1, keepdims=True)
            if h == 0:
                mine = jnp.where(left, packed[:quarter], turned[quarter:])
                line = jnp.where(left, target, pltpu.roll(diag, HALF, 1))
            else:
                mine = jnp.where(left, turned[:quarter], packed[quarter:])
                line = jnp.where(left, pltpu.roll(target, side, 1), pltpu.roll(diag, lanes - HALF, 1))
            packed_ref[p * quarter : (p + 1) * quarter, :] = mine
            at = owned * quarter + p
            packed_ref[at : at + 1, :] = line
            facts = jnp.where(lane == side, logs[h] / columns, line)
            facts = jnp.where(lane == side + 1, energy - quads[h], facts)
            facts = jnp.where(lane == side + 2, count, facts)
            facts_ref[p : p + 1, :] = facts


def total(x):
    return jnp.sum(jnp.sum(x, axis=0, keepdims=True), axis=1, keepdims=True)


def split(x):
    high = x.astype(jnp.bfloat16)
    return high, (x - high.astype(jnp.float32)).astype(jnp.bfloat16)


def conjugate(all_ref, coupling_ref, spectrum_ref, turned_ref, blocks_ref, w_ref, devices, owned):
    number = devices * owned
    rows = payload_rows(owned)
    quarter = HALF // 2
    fold = LANES // number

    def across(at):
        parts = [all_ref[pl.ds(begin, devices, stride=rows), :] for begin in at]
        return jnp.transpose(jnp.concatenate(parts * fold, axis=0))

    def turn(r, carry):
        x = across([h * quarter + r for h in range(owned)])
        turned_ref[pl.ds(pl.multiple_of(r * SIDE, SIDE), SIDE), :] = x[:SIDE]
        turned_ref[pl.ds(pl.multiple_of((r + quarter) * SIDE, SIDE), SIDE), :] = x[SIDE:]
        return carry

    for r in range(quarter):
        turn(r, 0)
    x = across([owned * quarter + h for h in range(owned)])
    target, diag = x[:SIDE], x[SIDE : SIDE + HALF]
    left = iota((HALF, LANES), 1) < SIDE
    sub = iota((HALF, LANES), 0)

    for r in range(HALF):
        mine = turned_ref[r * SIDE : r * SIDE + HALF, :]
        beside = turned_ref[r * SIDE + HALF : (r + 1) * SIDE, :]
        mirror = turned_ref[pl.ds(r, HALF, stride=SIDE), :]
        below = turned_ref[pl.ds(r + HALF, HALF, stride=SIDE), :]
        first = jnp.where(sub <= r, mine, mirror)
        last = jnp.where(sub > r, mine, jnp.where(sub == r, diag, mirror))
        if fold == 2:
            blocks_ref[r, 0:HALF, :] = jnp.where(left, first, below)
            blocks_ref[r, HALF:SIDE, :] = jnp.where(left, beside, last)
        else:
            blocks_ref[r, 0:HALF, :] = first
            blocks_ref[r, HALF:SIDE, :] = beside
            blocks_ref[r + HALF, 0:HALF, :] = below
            blocks_ref[r + HALF, HALF:SIDE, :] = last

    coupling = coupling_ref[...]
    row, col = iota(coupling.shape, 0), iota(coupling.shape, 1)
    high, low = split(jnp.where(row == lax.rem(col, number), 0.0, coupling))
    freqs = spectrum_ref.shape[1]
    place = jnp.where(iota((SIDE, freqs), 0) // 2 == iota((SIDE, freqs), 1), 1.0 / spectrum_ref[...], 0.0)
    power = dot(place, jnp.ones((freqs, LANES), jnp.float32))
    wide = iota((SIDE, LANES), 1) < SIDE

    def mix(v):
        top, rest = split(v)
        if fold == 2:
            x = jnp.where(wide, top.astype(jnp.float32), rest.astype(jnp.float32)).astype(jnp.bfloat16)
            out = jnp.dot(
                jnp.concatenate([x, x], axis=1),
                jnp.concatenate([high, high, low, low], axis=0),
                preferred_element_type=jnp.float32,
            )
        else:
            x = jnp.concatenate([top, rest], axis=1)
            out = jnp.dot(x, jnp.concatenate([high, high], axis=0), preferred_element_type=jnp.float32)
            out = out + jnp.dot(x, jnp.concatenate([low, low], axis=0), preferred_element_type=jnp.float32)
        return power * out

    def apply_blocks(v):
        if fold == 2:
            w_ref[0:HALF, :] = jnp.where(left, v[:HALF], v[HALF:])
        else:
            w_ref[...] = v
        acc = jnp.zeros((SIDE, LANES), jnp.float32)
        for k in range(SIDE // fold):
            acc = acc + blocks_ref[k] * w_ref[k : k + 1, :]
        return acc + pltpu.roll(acc, SIDE, 1) if fold == 2 else acc

    residual = target
    scaled = apply_blocks(residual)
    inner = total(residual * scaled)
    mixed = mix(scaled)
    solved = apply_blocks(mixed)
    direction, block_direction = scaled, residual
    solution = jnp.zeros((SIDE, LANES), jnp.float32)
    for iteration in range(ITERS):
        mapped = block_direction + mixed
        step = inner / total(direction * mapped)
        solution = solution + step * direction
        if iteration + 1 == ITERS:
            break
        residual = residual - step * mapped
        scaled = scaled - step * (direction + solved)
        following = total(residual * scaled)
        ratio = following / inner
        fresh = mix(scaled)
        if iteration + 2 < ITERS:
            solved = apply_blocks(fresh) + ratio * solved
        mixed = fresh + ratio * mixed
        direction = scaled + ratio * direction
        block_direction = residual + ratio * block_direction
        inner = following
    return solution


def gather_kernel(
    groups, chips, sums_ref, early_ref, prior_ref, coupling_ref, spectrum_ref, out_ref,
    mine_ref, facts_ref, all_ref, turned_ref, blocks_ref, w_ref, final_ref, psr_send, chip_send, core_send, recv
):
    psr, me = lax.axis_index("psr"), lax.axis_index("toa")
    toa_devices = 2 * chips
    devices = groups * toa_devices
    core = lax.rem(me, 2)
    chip = me // 2
    other = 1 - core
    partner = chip * 2 + other
    rows = mine_ref.shape[0]
    owned = out_ref.shape[0]
    barrier = pltpu.get_barrier_semaphore()

    def greet(psr_to, toa_to):
        pl.semaphore_signal(barrier, inc=1, device_id={"psr": psr_to, "toa": toa_to}, device_id_type=MESH)

    greet(psr, partner)
    for d in range(1, chips):
        greet(psr, lax.rem(chip + d, chips) * 2 + core)
    for e in range(1, groups):
        greet(lax.rem(psr + e, groups), me)
    own = psr * toa_devices + me
    eliminate(devices, own, sums_ref, early_ref, prior_ref, coupling_ref, spectrum_ref, mine_ref, facts_ref)
    pl.semaphore_wait(barrier, chips + groups - 1)
    sent = []

    def block_of(e, toa):
        return lax.rem(psr + groups - e, groups) * toa_devices + toa

    def slot(block):
        return all_ref.at[pl.ds(pl.multiple_of(block * rows, 8), rows)]

    def copy(source, block, sem, psr_to, toa_to):
        return pltpu.make_async_remote_copy(
            src_ref=source,
            dst_ref=slot(block),
            send_sem=sem,
            recv_sem=recv.at[block],
            device_id={"psr": psr_to, "toa": toa_to},
            device_id_type=MESH,
        )

    def send(source, block, sem, psr_to, toa_to):
        moving = copy(source, block, sem, psr_to, toa_to)
        moving.start()
        sent.append(moving)

    def arrived(block):
        copy(slot(block), block, core_send.at[0], psr, partner).wait_recv()

    for e in range(1, groups):
        send(mine_ref, own, psr_send.at[e - 1], lax.rem(psr + e, groups), me)
    for e in range(groups):
        block = block_of(e, me)
        if e:
            arrived(block)
        source = slot(block) if e else mine_ref
        for d in range(1, chips):
            send(source, block, chip_send.at[e * (chips - 1) + d - 1], psr, lax.rem(chip + d, chips) * 2 + core)
        send(source, block, core_send.at[e], psr, partner)
    for d in range(1, chips):
        for e in range(groups):
            block = block_of(e, lax.rem(chip + chips - d, chips) * 2 + core)
            arrived(block)
            send(slot(block), block, core_send.at[d * groups + e], psr, partner)
    all_ref[pl.ds(pl.multiple_of(own * rows, 8), rows), :] = mine_ref[...]
    for c in range(chips):
        for e in range(groups):
            arrived(block_of(e, c * 2 + other))
    for moving in sent:
        moving.wait_send()
    solution = conjugate(all_ref, coupling_ref, spectrum_ref, turned_ref, blocks_ref, w_ref, devices, owned)
    final_ref[...] = jnp.transpose(jnp.concatenate([solution, solution], axis=0))
    lane = iota((1, LANES), 1)
    for h in range(owned):
        mine = final_ref[pl.ds(h * devices + own, 1), :]
        facts = facts_ref[h : h + 1, :]
        fit = jnp.sum(jnp.where(lane < SIDE, facts * mine, 0.0), axis=1, keepdims=True)

        def at(k):
            return jnp.sum(jnp.where(lane == SIDE + k, facts, 0.0), axis=1, keepdims=True)

        chi_square = (at(1) - fit) / at(2)
        line = jnp.where(lane < SIDE, mine, jnp.where(lane == SIDE, at(0), chi_square))
        out_ref[h : h + 1, :] = line


def finish(sums, early, own_prior, coupling, spectrum, groups, toa_devices):
    chips = toa_devices // 2
    devices = groups * toa_devices
    owned = sums.shape[0]
    rows = payload_rows(owned)
    fold = LANES // (devices * owned)
    vmem = pl.BlockSpec(memory_space=pltpu.VMEM)
    return pl.pallas_call(
        functools.partial(gather_kernel, groups, chips),
        out_shape=jax.ShapeDtypeStruct((owned, LANES), jnp.float32),
        in_specs=[vmem] * 5,
        out_specs=vmem,
        scratch_shapes=[
            pltpu.VMEM((rows, LANES), jnp.float32),
            pltpu.VMEM((owned, LANES), jnp.float32),
            pltpu.VMEM((devices * rows, LANES), jnp.float32),
            pltpu.VMEM((HALF * SIDE, LANES), jnp.float32),
            pltpu.VMEM((SIDE // fold, SIDE, LANES), jnp.float32),
            pltpu.VMEM((SIDE, LANES), jnp.float32),
            pltpu.VMEM((LANES, LANES), jnp.float32),
            pltpu.SemaphoreType.DMA((groups - 1,)),
            pltpu.SemaphoreType.DMA((groups * (chips - 1),)),
            pltpu.SemaphoreType.DMA((groups * chips,)),
            pltpu.SemaphoreType.DMA((devices,)),
        ],
        compiler_params=pltpu.CompilerParams(collective_id=1, has_side_effects=True, vmem_limit_bytes=20 * 2**20),
        name="finish",
    )(sums, early, own_prior, coupling, spectrum)


def body(design, noise_weight, residuals, slot_pulsar, slot_rows, own_prior, spectrum, directions):
    groups, toa_devices = lax.axis_size("psr"), lax.axis_size("toa")
    partial = local_grams(design, noise_weight, residuals, slot_pulsar, slot_rows)
    sums, coupling, early = reduce_owners(partial, directions, own_prior, toa_devices)
    lines = finish(sums, early, own_prior, coupling, spectrum[None, :], groups, toa_devices)
    return (lines[:, :SIDE], lines[:, SIDE], lines[:, SIDE + 1])


def solution(mesh):
    return jax.shard_map(
        body,
        mesh=mesh,
        in_specs=(
            P(("psr", "toa"), None, None),
            P(("psr", "toa"), None),
            P(("psr", "toa"), None),
            P(("psr", "toa")),
            P(("psr", "toa")),
            P(("psr", "toa"), None),
            P(),
            P(),
        ),
        out_specs=(P(("psr", "toa"), None), P(("psr", "toa")), P(("psr", "toa"))),
        check_vma=False,
    )
```
